32 devices in a mesh: comp: 2 (over core), dom: 16 (over z, y, x).
Axes of the slice: x: 2, y: 2, z: 4, core: 2. Of those that a mesh axis runs over, the one named last changes fastest.
Arguments:
- surface_flux: float32 [6, 12, 131072], P(None, None, ('comp', 'dom')), may hold values from -8 to 8
- active_mask: int32 [131072], P(('comp', 'dom')), may hold values 0 or 1
- source_area: float32 [131072], P(('comp', 'dom')), may hold values from 0.5 to 30
- tile_targets: int32 [2048, 2], P(('comp', 'dom')), may hold values from 0 to 31, all different within a row
- remap_tiles: float32 [2048, 2, 64, 384], P(('comp', 'dom')), may hold values from -0.0625 to 0.0625
- ocean_flux: float32 [12, 12288], P(None, ('comp', 'dom')), may hold values from -6 to 6
- air_fraction: float32 [3, 12288], P(None, ('comp', 'dom')), may hold values from 0 to 1, as said below
- air_area: float32 [12288], P(('comp', 'dom')), may hold values from 0.5 to 30
Outputs:
- merged: float32 [12, 12288], P(None, ('comp', 'dom'))
- area_means: float32 [3, 12], replicated
The draws below stay inside these ranges and needn't reach their ends.
Inputs may be any that keep to these rules, and one draw needn't show every extreme that they name: `air_fraction`: the three fractions of a cell are positive and sum to one. `tile_targets`: the 2 targets of one source block differ.
All inputs are finite; a program needn't handle non-finite values. No bound on the sum of `active_mask` on one device may be relied on, other than what follows from the above.
Results may differ from the reference program's by a relative error of at most 0.000071.
Values sent between devices are 32-bit elements; how exact they have to be, the bound alone decides.
A program may use at most 64 MiB of HBM per device.

```python
import math
import jax
import jax.numpy as jnp
from jax import lax

FIELDS = 12
STEPS = 6
TOP = 2
BS = 64
SBLK = 64
ATM_DEV = 384
BLOCKS = 2048
SRC_CELLS = 131072
ATM_CELLS = 12288
N_COMP = 2
N_DOM = 16


def draw_surface_flux(key, part):
    subkeys = jax.random.split(key, 4)
    position = jnp.arange(SRC_CELLS, dtype=jnp.float32) / SRC_CELLS
    amplitude = jax.random.uniform(subkeys[0], (FIELDS, 1), jnp.float32, 0.5, 1.5)
    phase = jax.random.uniform(subkeys[1], (FIELDS, 1), jnp.float32, 0.0, 2.0 * math.pi)
    waves = 1.0 + (jnp.arange(FIELDS, dtype=jnp.int32) % 3).astype(jnp.float32)[:, None]
    offset = jax.random.uniform(subkeys[2], (FIELDS, 1), jnp.float32, -0.5, 0.5)
    trend = amplitude * jnp.cos(math.pi * waves * position[None, :] + phase) + offset
    noise = jax.random.normal(subkeys[3], (STEPS, FIELDS, SRC_CELLS), jnp.float32)
    return jnp.clip(trend[None, :, :] + noise, -8.0, 8.0)


def rising_area(key, total_cells):
    position = jnp.arange(total_cells, dtype=jnp.float32) / total_cells
    factor = jax.random.uniform(key, (total_cells,), jnp.float32, 0.5, 1.5)
    return (1.0 + 2.0 * position) * factor


def draw_source_area(key, part):
    return rising_area(jax.random.fold_in(key, 11), SRC_CELLS)


def draw_air_area(key, part):
    return rising_area(jax.random.fold_in(key, 23), ATM_CELLS)


def draw_air_fraction(key, part):
    shares = jax.random.uniform(key, (3, ATM_CELLS), jnp.float32, 0.1, 1.0)
    return shares / jnp.sum(shares, axis=0, keepdims=True)


def place_ends(result, key, smallest, largest):
    longest = result.shape.index(max(result.shape))
    spots = []
    for shift in (0, 1):
        where = [jax.random.randint(jax.random.fold_in(key, axis), (), 0, length) for axis, length in enumerate(result.shape)]
        where[longest] = (where[longest] + shift) % result.shape[longest]
        spots.append(tuple(where))
    return result.at[spots[0]].set(smallest).at[spots[1]].set(largest)


def shard_levels(own_key, shape, shards, smallest, largest):
    def one(axis_at, shards_of):
        heights = jax.random.uniform(jax.random.fold_in(jax.random.fold_in(own_key, 6), axis_at), (shards_of,), jnp.float32, smallest / len(shards), largest / len(shards))
        return jnp.repeat(jnp.exp(heights), shape[axis_at] // shards_of).reshape((-1,) + (1,) * (len(shape) - axis_at - 1))

    level = one(*shards[0])
    for cut in shards[1:]:
        level = level * one(*cut)
    return level


def different_ones(own_key, rows, number_of, top, lift):
    sequence = jax.random.permutation(jax.random.fold_in(own_key, 1), number_of)
    favour = sequence
    for power in range(3):
        favour = favour * favour // number_of
    favour = favour * lift // number_of
    lots = jax.random.randint(jax.random.fold_in(own_key, 2), (rows, number_of), 0, 4096) + favour
    holders = jax.random.permutation(jax.random.fold_in(own_key, 3), rows)[jnp.arange(number_of) % rows]
    lots = jnp.where(jnp.arange(rows)[:, None] == holders[None, :], 1 << 14, lots)
    priority = lots * number_of + jnp.arange(number_of)
    return lax.top_k(priority.astype(jnp.int32), top)[1].astype(jnp.int32)


def normal_values(rng, extent, spread, bound, cuts=(), kind=jnp.bfloat16):
    loudness = shard_levels(rng, extent, cuts, -0.22, 0.18) if cuts else 1.0
    result = jax.random.normal(rng, extent, jnp.float32) * spread * loudness
    return jnp.minimum(jnp.maximum(result, -bound), bound).astype(kind)


def setup_inputs(seed: int = 0) -> dict:
    streams_of = jax.random.split(jax.random.key(seed), 9)
    return {
        "surface_flux": draw_surface_flux(jax.random.fold_in(streams_of[8], 71), 0),
        "active_mask": place_ends((jax.random.randint(streams_of[1], (SRC_CELLS,), 0, 4) < 3).astype(jnp.int32), jax.random.fold_in(streams_of[1], 1), 0, 1),
        "source_area": draw_source_area(jax.random.fold_in(streams_of[8], 71), 0),
        "tile_targets": different_ones(streams_of[3], BLOCKS, N_COMP * N_DOM, TOP, 0),
        "remap_tiles": normal_values(streams_of[4], (BLOCKS, TOP, BS, ATM_DEV), (BS * SBLK * TOP) ** -0.5, 0.0625, ((0, 32),), jnp.float32),
        "ocean_flux": normal_values(streams_of[5], (FIELDS, ATM_CELLS), 1.0, 6.0, ((1, 32),), jnp.float32),
        "air_fraction": draw_air_fraction(jax.random.fold_in(streams_of[8], 71), 0),
        "air_area": draw_air_area(jax.random.fold_in(streams_of[8], 71), 0),
    }


def reference(surface_flux, active_mask, source_area, tile_targets, remap_tiles, ocean_flux, air_fraction, air_area):
    average = jnp.sum(surface_flux, axis=0) / STEPS
    weighted = average * (active_mask.astype(jnp.float32) * source_area)[None, :]
    blocks = weighted.reshape(FIELDS, BLOCKS, BS)
    contrib = jnp.einsum("fbs,btsa->btfa", blocks, remap_tiles, precision=lax.Precision.HIGHEST)
    contrib = contrib.reshape(BLOCKS * TOP, FIELDS, ATM_DEV)
    owner_total = N_COMP * N_DOM
    comp_of_block = (jnp.arange(BLOCKS, dtype=jnp.int32) // (SBLK * N_DOM)).astype(jnp.int32)
    segment = (comp_of_block[:, None] * owner_total + tile_targets).reshape(BLOCKS * TOP).astype(jnp.int32)
    summed = jax.ops.segment_sum(contrib, segment, num_segments=N_COMP * owner_total)
    summed = summed.reshape(N_COMP, owner_total, FIELDS, ATM_DEV).transpose(0, 2, 1, 3)
    remapped = summed.reshape(N_COMP, FIELDS, ATM_CELLS) / air_area[None, None, :]
    merged = air_fraction[0][None, :] * remapped[0] + air_fraction[1][None, :] * remapped[1] + air_fraction[2][None, :] * ocean_flux
    surface_num = jnp.sum(weighted.reshape(FIELDS, N_COMP, SRC_CELLS // N_COMP), axis=2).T
    surface_den = jnp.sum(source_area.reshape(N_COMP, SRC_CELLS // N_COMP), axis=1)
    air_num = jnp.sum(merged * air_area[None, :], axis=1)
    air_den = jnp.sum(air_area)
    area_means = jnp.concatenate([surface_num / surface_den[:, None], (air_num / air_den)[None, :]], axis=0)
    return merged, area_means
```

```python
import functools

import jax
import jax.numpy as jnp
from jax import lax
from jax.experimental import pallas as pl
from jax.experimental.pallas import tpu as pltpu
from jax.sharding import PartitionSpec as P

MESH = pl.DeviceIdType.MESH
F32 = jnp.float32
BF16 = jnp.bfloat16
AHEAD = 2
SEND_ROWS_AT = 4
FLUX_PARTS = 4
UNROLL = 4
PAIR_CUTS = 3


def split(x):
    hi = x.astype(BF16)
    lo = (x - hi.astype(F32)).astype(BF16)
    return hi, lo


def chunk_sizes(blocks):
    whole = blocks // 8
    return [whole] * 7 + [whole // 2] * 2


def kernel(
    groups,
    domains,
    flux_hbm,
    mask_hbm,
    area_hbm,
    targets_hbm,
    tiles_hbm,
    ocean_hbm,
    fraction_hbm,
    air_hbm,
    merged_ref,
    means_ref,
    flux,
    mask,
    area,
    targets,
    tiles,
    ocean,
    fraction,
    air,
    stacked,
    lhs,
    contrib,
    picks,
    row_out,
    rows_in,
    summed,
    air_parts,
    partner_in,
    stat_out,
    stat_in,
    outgoing,
    incoming,
    flux_sem,
    tile_sem,
    small_sem,
    row_send,
    row_recv,
    pair_send,
    pair_recv,
    stat_send,
    stat_recv,
    main_send,
    main_recv,
):
    steps, fields, cells = flux.shape
    blocks, slots, block_cells, air_cells = tiles.shape
    owners = groups * domains
    chunks = chunk_sizes(blocks)
    lane_tiles = air_cells // 128
    tile_count = blocks * slots
    body_rows = lane_tiles * fields
    comp = lax.axis_index("comp")
    dom = lax.axis_index("dom")
    other = 1 - comp

    small = [
        pltpu.make_async_copy(src, dst, small_sem.at[i])
        for i, (src, dst) in enumerate(
            [
                (fraction_hbm, fraction),
                (mask_hbm, mask),
                (area_hbm, area),
                (targets_hbm, targets),
                (ocean_hbm, ocean),
                (air_hbm, air),
            ]
        )
    ]
    for copy in small[:3]:
        copy.start()
    flux_width = cells // FLUX_PARTS
    flux_copies = []
    for i in range(FLUX_PARTS):
        part = pl.ds(i * flux_width, flux_width)
        copy = pltpu.make_async_copy(
            flux_hbm.at[:, :, part], flux.at[:, :, part], flux_sem.at[i]
        )
        copy.start()
        flux_copies.append(copy)
    tile_copies = []
    low = 0
    for i, size in enumerate(chunks):
        part = pl.ds(low, size)
        low += size
        tile_copies.append(
            pltpu.make_async_copy(tiles_hbm.at[part], tiles.at[part], tile_sem.at[i])
        )
    waiting = list(tile_copies)

    def start_more(count):
        for copy in waiting[:count]:
            copy.start()
        del waiting[:count]

    start_more(AHEAD)

    barrier = pltpu.get_barrier_semaphore()
    rivals = []
    for k in range(domains - 1):
        rivals.append((comp, k + jnp.where(dom <= k, 1, 0)))
    mates = [(other, k) for k in range(domains)]
    for a, b in zip(rivals + [None], mates):
        for peer in (a, b):
            if peer is not None:
                pl.semaphore_signal(barrier, inc=1, device_id=peer, device_id_type=MESH)

    small[1].wait()
    small[2].wait()
    width = min(512, flux_width)
    lane = lax.broadcasted_iota(jnp.int32, (fields, width), 1)
    first = lax.rem(lane, 2 * block_cells) < block_cells

    def weigh(i, carry):
        total, area_total = carry
        part = pl.ds(pl.multiple_of(i * width, width), width)
        value = flux[0, :, part]
        for s in range(1, steps):
            value = value + flux[s, :, part]
        a = area[:, part]
        value = (value / steps) * (mask[:, part].astype(F32) * a)
        stacked[pl.ds(0, fields), part] = jnp.where(first, value, 0.0)
        stacked[pl.ds(fields, fields), part] = jnp.where(first, 0.0, value)
        both = stacked[:, part]
        hi = both.astype(BF16).astype(F32)
        left = jnp.concatenate([hi, both - hi], axis=0).astype(BF16)
        right = jnp.concatenate([hi, jnp.zeros_like(hi)], axis=0).astype(BF16)
        for j in range(width // 128):
            cut = slice(j * 128, (j + 1) * 128)
            base = pl.multiple_of(2 * i * width + 256 * j, 256)
            lhs[:, pl.ds(base, 128)] = left[:, cut]
            lhs[:, pl.ds(base + 128, 128)] = right[:, cut]
        return total + value, area_total + a

    carry = (jnp.zeros((fields, width), F32), jnp.zeros((1, width), F32))
    rounds = flux_width // width
    for i in range(FLUX_PARTS):
        flux_copies[i].wait()
        start_more(1)
        carry = lax.fori_loop(i * rounds, (i + 1) * rounds, weigh, carry, unroll=rounds)
    surface_num = jnp.sum(carry[0], axis=1, keepdims=True)
    surface_den = jnp.sum(carry[1])

    def pair(j, carry):
        left = lhs[:, pl.ds(pl.multiple_of(j * 256, 256), 256)]
        right = []
        for t in range(slots):
            weights = tiles[pl.ds(2 * j, 2), t].reshape(2 * block_cells, air_cells)
            hi, lo = split(weights)
            right.append(jnp.concatenate([hi, lo], axis=0))
        r = jnp.dot(left, jnp.concatenate(right, axis=1), preferred_element_type=F32)
        r = r[: 2 * fields] + r[2 * fields :]
        for t in range(slots):
            base = pl.multiple_of((t * blocks + 2 * j) * fields, 2 * fields)
            for q in range(lane_tiles):
                n = t * lane_tiles + q
                contrib[q, pl.ds(base, 2 * fields), :] = r[:, n * 128 : (n + 1) * 128]
        return carry

    def row_copy(p, slot):
        return pltpu.make_async_remote_copy(
            src_ref=row_out,
            dst_ref=rows_in.at[pl.ds(pl.multiple_of(slot * 8, 8), groups * lane_tiles)],
            send_sem=row_send,
            recv_sem=row_recv,
            device_id=(comp, p),
            device_id_type=MESH,
        )

    low = 0
    for i, size in enumerate(chunks):
        if i == SEND_ROWS_AT:
            small[0].wait()
            for c in range(groups):
                for q in range(lane_tiles):
                    row = fraction[pl.ds(c, 1), pl.ds(q * 128, 128)]
                    row_out[pl.ds(c * lane_tiles + q, 1), :] = row
                    rows_in[pl.ds(dom * 8 + c * lane_tiles + q, 1), :] = row
            pl.semaphore_wait(barrier, owners - 1)
            for c, p in rivals:
                row_copy(p, dom).start()
        tile_copies[i].wait()
        start_more(1)
        if i == 3:
            for copy in small[3:]:
                copy.start()
        pairs = size // 2
        lax.fori_loop(low, low + pairs, pair, 0, unroll=min(UNROLL, pairs))
        low += pairs

    small[3].wait()
    picks[:, pl.ds(0, blocks)] = targets[...]
    picks[:, pl.ds(blocks, blocks)] = targets[...]
    picked = jnp.where(
        lax.broadcasted_iota(jnp.int32, (1, tile_count), 1) < blocks,
        picks[pl.ds(0, 1), :],
        picks[pl.ds(1, 1), :],
    )
    owner_ids = lax.broadcasted_iota(jnp.int32, (owners, tile_count), 0)
    selector = jnp.where(owner_ids == picked, 1.0, 0.0).astype(BF16)
    selector = jnp.concatenate([selector, selector], axis=1)

    def collect(g, carry):
        right = []
        for f in (2 * g, 2 * g + 1):
            for q in range(lane_tiles):
                hi, lo = split(contrib[q, pl.ds(f, tile_count, stride=fields), :])
                right.append(jnp.concatenate([hi, lo], axis=0))
        s = jnp.dot(selector, jnp.concatenate(right, axis=1), preferred_element_type=F32)
        for n, f in enumerate((2 * g, 2 * g + 1)):
            summed[f] = s[:, n * air_cells : (n + 1) * air_cells]
        return carry

    far = pl.ds(pl.multiple_of(other * domains, 8), domains)
    own = pl.ds(pl.multiple_of(comp * domains, 8), domains)
    per_cut = fields // PAIR_CUTS
    pair_copies = []
    for n in range(PAIR_CUTS):
        lax.fori_loop(n * per_cut // 2, (n + 1) * per_cut // 2, collect, 0, unroll=per_cut // 2)
        part = pl.ds(n * per_cut, per_cut)
        copy = pltpu.make_async_remote_copy(
            src_ref=summed.at[part, far],
            dst_ref=partner_in.at[part],
            send_sem=pair_send.at[n],
            recv_sem=pair_recv.at[n],
            device_id=(other, dom),
            device_id_type=MESH,
        )
        copy.start()
        pair_copies.append(copy)

    small[4].wait()
    small[5].wait()
    air_row = air[...].reshape(1, air_cells)
    inverse = 1.0 / air_row
    ocean_part = fraction[pl.ds(2, 1), :] * ocean[...]
    wet = air_row * ocean_part
    wet = sum(wet[:, q * 128 : (q + 1) * 128] for q in range(lane_tiles))
    air_den = jnp.sum(air_row)
    spot = lax.broadcasted_iota(jnp.int32, (fields, 128), 1)
    line = lax.broadcasted_iota(jnp.int32, (fields, 128), 0)
    stat = jnp.where(spot == line + 16 * comp, surface_num, 0.0)
    stat = jnp.sum(stat, axis=0, keepdims=True)
    spot1 = lax.broadcasted_iota(jnp.int32, (1, 128), 1)
    lead = spot1 - 64
    stat = stat + jnp.where((lead >= 16 * comp) & (lead < 16 * comp + 16), surface_den, 0.0)
    stat = stat + jnp.where(
        (lead >= 16 * groups) & (lead < 16 * groups + 16), air_den, 0.0
    )

    pltpu.make_async_remote_copy(
        src_ref=rows_in.at[pl.ds(0, (domains - 1) * groups * lane_tiles)],
        dst_ref=rows_in.at[pl.ds(0, (domains - 1) * groups * lane_tiles)],
        send_sem=row_send,
        recv_sem=row_recv,
        device_id=(other, dom),
        device_id_type=MESH,
    ).wait_recv()

    def shares(c):
        return [
            rows_in[pl.ds(c * lane_tiles + q, domains, stride=8), :]
            for q in range(lane_tiles)
        ]

    share_own = shares(comp)
    share_other = shares(other)

    def main_copy(p, slot):
        return pltpu.make_async_remote_copy(
            src_ref=outgoing.at[p, pl.ds(0, body_rows + 1)],
            dst_ref=incoming.at[slot, pl.ds(0, body_rows + 1)],
            send_sem=main_send,
            recv_sem=main_recv.at[slot],
            device_id=(comp, p),
            device_id_type=MESH,
        )

    def stat_copy(p, slot):
        return pltpu.make_async_remote_copy(
            src_ref=stat_out,
            dst_ref=stat_in.at[slot],
            send_sem=stat_send,
            recv_sem=stat_recv,
            device_id=(other, p),
            device_id_type=MESH,
        )

    for n in range(PAIR_CUTS):
        pair_copies[n].wait_recv()
        for f in range(n * per_cut, (n + 1) * per_cut):
            acc = None
            for q in range(lane_tiles):
                cut = pl.ds(q * 128, 128)
                both = share_own[q] * summed[f, own, cut]
                both = both + share_other[q] * partner_in[f, :, cut]
                outgoing[:, q * fields + f, :] = both
                acc = both if acc is None else acc + both
            air_parts[pl.ds(f, 1), :] = jnp.sum(acc, axis=0, keepdims=True)
    air_num = jnp.sum(air_parts[...] + wet, axis=1, keepdims=True)
    air_num = jnp.where(spot == line + 16 * groups, air_num, 0.0)
    stat = stat + jnp.sum(air_num, axis=0, keepdims=True)
    outgoing[:, body_rows, :] = jnp.broadcast_to(stat, (domains, 128))
    stat_out[...] = stat
    for k in range(domains):
        stat_copy(k, dom).start()
    for c, p in rivals:
        main_copy(p, dom).start()

    sums = []
    for q in range(lane_tiles):
        sums.append(outgoing[dom, pl.ds(q * fields, fields), :])
    for c, p in rivals:
        main_copy(p, p).wait_recv()
        for q in range(lane_tiles):
            sums[q] = sums[q] + incoming[p, pl.ds(q * fields, fields), :]
        stat = stat + incoming[p, pl.ds(body_rows, 1), :]
    for q in range(lane_tiles):
        cut = slice(q * 128, (q + 1) * 128)
        merged_ref[:, cut] = sums[q] * inverse[:, cut] + ocean_part[:, cut]

    pltpu.make_async_remote_copy(
        src_ref=stat_in,
        dst_ref=stat_in,
        send_sem=stat_send,
        recv_sem=stat_recv,
        device_id=(other, dom),
        device_id_type=MESH,
    ).wait_recv()
    stat = stat + jnp.sum(stat_in[...], axis=0)
    mean = stat / pltpu.roll(stat, 64, 1)
    for c in range(groups + 1):
        moved = mean if c == 0 else pltpu.roll(mean, 128 - 16 * c, 1)
        means_ref[pl.ds(c, 1), :] = moved[:, :fields]

    pltpu.make_async_remote_copy(
        src_ref=rows_in.at[pl.ds(0, (domains - 1) * groups * lane_tiles)],
        dst_ref=rows_in.at[pl.ds(0, (domains - 1) * groups * lane_tiles)],
        send_sem=row_send,
        recv_sem=row_recv,
        device_id=(other, dom),
        device_id_type=MESH,
    ).wait_send()
    for copy in pair_copies:
        copy.wait_send()
    pltpu.make_async_remote_copy(
        src_ref=stat_in,
        dst_ref=stat_in,
        send_sem=stat_send,
        recv_sem=stat_recv,
        device_id=(other, dom),
        device_id_type=MESH,
    ).wait_send()
    pltpu.make_async_remote_copy(
        src_ref=outgoing.at[pl.ds(0, domains - 1), pl.ds(0, body_rows + 1)],
        dst_ref=outgoing.at[pl.ds(0, domains - 1), pl.ds(0, body_rows + 1)],
        send_sem=main_send,
        recv_sem=main_recv.at[0],
        device_id=(other, dom),
        device_id_type=MESH,
    ).wait_send()


def finish(merged_in, means_in, merged_ref, means_ref):
    merged_ref[...] = merged_in[...]
    means_ref[...] = means_in[...]


def on_device(
    surface_flux,
    active_mask,
    source_area,
    tile_targets,
    remap_tiles,
    ocean_flux,
    air_fraction,
    air_area,
):
    groups = lax.axis_size("comp")
    domains = lax.axis_size("dom")
    owners = groups * domains
    fields = surface_flux.shape[1]
    cells = surface_flux.shape[2]
    blocks, slots, block_cells, air_cells = remap_tiles.shape
    lane_tiles = air_cells // 128
    message = -(-(lane_tiles * fields + 1) // 8) * 8
    vmem = pl.BlockSpec(memory_space=pltpu.VMEM)
    hbm = pl.BlockSpec(memory_space=pltpu.HBM)
    dma = pltpu.SemaphoreType.DMA
    parts = pl.pallas_call(
        functools.partial(kernel, groups, domains),
        out_shape=(
            pltpu.VMEM((fields, air_cells), F32),
            pltpu.VMEM((groups + 1, fields), F32),
        ),
        in_specs=[hbm] * 8,
        out_specs=(vmem, vmem),
        scratch_shapes=[
            pltpu.VMEM(surface_flux.shape, F32),
            pltpu.VMEM((1, cells), jnp.int32),
            pltpu.VMEM((1, cells), F32),
            pltpu.VMEM((slots, blocks), jnp.int32),
            pltpu.VMEM(remap_tiles.shape, F32),
            pltpu.VMEM(ocean_flux.shape, F32),
            pltpu.VMEM(air_fraction.shape, F32),
            pltpu.VMEM((air_cells,), F32),
            pltpu.VMEM((2 * fields, cells), F32),
            pltpu.VMEM((4 * fields, 2 * cells), BF16),
            pltpu.VMEM((lane_tiles, blocks * slots * fields, 128), F32),
            pltpu.VMEM((slots, blocks * slots), jnp.int32),
            pltpu.VMEM((groups * lane_tiles, 128), F32),
            pltpu.VMEM((domains * 8, 128), F32),
            pltpu.VMEM((fields, owners, air_cells), F32),
            pltpu.VMEM((fields, 128), F32),
            pltpu.VMEM((fields, domains, air_cells), F32),
            pltpu.VMEM((1, 128), F32),
            pltpu.VMEM((domains, 1, 128), F32),
            pltpu.VMEM((domains, message, 128), F32),
            pltpu.VMEM((domains, message, 128), F32),
            dma((FLUX_PARTS,)),
            dma((len(chunk_sizes(blocks)),)),
            dma((6,)),
            dma,
            dma,
            dma((PAIR_CUTS,)),
            dma((PAIR_CUTS,)),
            dma,
            dma,
            dma,
            dma((domains,)),
        ],
        compiler_params=pltpu.CompilerParams(
            collective_id=0, has_side_effects=True, vmem_limit_bytes=60 * 1024 * 1024
        ),
    )(
        surface_flux,
        active_mask.reshape(1, cells),
        source_area.reshape(1, cells),
        tile_targets.T,
        remap_tiles,
        ocean_flux,
        air_fraction,
        air_area,
    )
    return pl.pallas_call(
        finish,
        out_shape=(
            jax.ShapeDtypeStruct((fields, air_cells), F32),
            jax.ShapeDtypeStruct((groups + 1, fields), F32),
        ),
        in_specs=[vmem, vmem],
        out_specs=(vmem, vmem),
    )(*[pltpu.with_memory_space_constraint(p, pltpu.VMEM) for p in parts])


def solution(mesh):
    in_specs = (
        P(None, None, ("comp", "dom")),
        P(("comp", "dom")),
        P(("comp", "dom")),
        P(("comp", "dom"), None),
        P(("comp", "dom"), None, None, None),
        P(None, ("comp", "dom")),
        P(None, ("comp", "dom")),
        P(("comp", "dom")),
    )
    out_specs = (P(None, ("comp", "dom")), P())
    return jax.shard_map(
        on_device, mesh=mesh, in_specs=in_specs, out_specs=out_specs, check_vma=False
    )
```

```python
import functools

import jax
import jax.numpy as jnp
from jax import lax
from jax.experimental import pallas as pl
from jax.experimental.pallas import tpu as pltpu
from jax.sharding import PartitionSpec as P

MESH = pl.DeviceIdType.MESH
F32 = jnp.float32
BF16 = jnp.bfloat16
DEPTH = 8
EXTRA = 4
SEND_ROWS_AT = 2
PARTS = 4
UNROLL = 8
PAIR_CUTS = 3
AT_ONCE = 1
SIDE_AT = 1


def split(x):
    hi = x.astype(BF16)
    lo = (x - hi.astype(F32)).astype(BF16)
    return hi, lo


def plan(blocks):
    whole = blocks // PARTS
    copies = [[whole // 4] * 4] * PARTS
    rounds = [[whole // 2] * 2] + [[whole]] * (PARTS - 2) + [[whole // 2, whole // 4, whole // 4]]
    return copies, rounds


def kernel(
    groups,
    domains,
    flux_hbm,
    mask_hbm,
    area_hbm,
    targets_hbm,
    tiles_hbm,
    ocean_hbm,
    fraction_hbm,
    air_hbm,
    merged_ref,
    means_ref,
    flux,
    mask,
    area,
    targets,
    tiles,
    ocean,
    fraction,
    air,
    stacked,
    lhs,
    contrib,
    picks,
    row_out,
    rows_in,
    summed,
    air_parts,
    partner_in,
    stat_out,
    stat_in,
    outgoing,
    incoming,
    relayed,
    flux_sem,
    tile_sem,
    small_sem,
    row_send,
    row_recv,
    pair_send,
    pair_recv,
    stat_send,
    stat_recv,
    main_send,
    main_recv,
):
    steps, fields, cells = flux.shape
    blocks, slots, block_cells, air_cells = tiles.shape
    owners = groups * domains
    copy_plan, round_plan = plan(blocks)
    lane_tiles = air_cells // 128
    body_rows = lane_tiles * fields
    comp = lax.axis_index("comp")
    dom = lax.axis_index("dom")
    other = 1 - comp

    small = [
        pltpu.make_async_copy(src, dst, small_sem.at[i])
        for i, (src, dst) in enumerate(
            [
                (fraction_hbm, fraction),
                (mask_hbm, mask),
                (area_hbm, area),
                (targets_hbm, targets),
                (ocean_hbm, ocean),
                (air_hbm, air),
            ]
        )
    ]
    for copy in small[1:3]:
        copy.start()
    flux_width = cells // PARTS
    flux_copies = []
    tile_copies = []
    waiting = []
    low = 0
    for i in range(PARTS):
        part = pl.ds(i * flux_width, flux_width)
        flux_copies.append(
            pltpu.make_async_copy(flux_hbm.at[:, :, part], flux.at[:, :, part], flux_sem.at[i])
        )
        for size in copy_plan[i]:
            part = pl.ds(low, size)
            low += size
            copy = pltpu.make_async_copy(
                tiles_hbm.at[part], tiles.at[part], tile_sem.at[len(tile_copies)]
            )
            tile_copies.append((low, copy))
            waiting.append(copy)

    def start_more(count):
        for copy in waiting[:count]:
            copy.start(priority=1)
        del waiting[:count]

    flux_copies[0].start()
    start_more(DEPTH)
    flux_copies[1].start()
    small[0].start()

    barrier = pltpu.get_barrier_semaphore()
    rivals = []
    for k in range(domains - 1):
        rivals.append((comp, k + jnp.where(dom <= k, 1, 0)))
    mates = [(other, k) for k in range(domains)]
    for a, b in zip(rivals + [None], mates):
        for peer in (a, b):
            if peer is not None:
                pl.semaphore_signal(barrier, inc=1, device_id=peer, device_id_type=MESH)

    small[1].wait()
    small[2].wait()
    width = min(512, flux_width)
    lane = lax.broadcasted_iota(jnp.int32, (fields, width), 1)
    first = lax.rem(lane, 2 * block_cells) < block_cells

    def weigh(i, carry):
        total, area_total = carry
        part = pl.ds(pl.multiple_of(i * width, width), width)
        value = flux[0, :, part]
        for s in range(1, steps):
            value = value + flux[s, :, part]
        a = area[:, part]
        value = (value / steps) * (mask[:, part].astype(F32) * a)
        stacked[pl.ds(0, fields), part] = jnp.where(first, value, 0.0)
        stacked[pl.ds(fields, fields), part] = jnp.where(first, 0.0, value)
        both = stacked[:, part]
        hi = both.astype(BF16).astype(F32)
        left = jnp.concatenate([hi, both - hi], axis=0).astype(BF16)
        right = jnp.concatenate([hi, jnp.zeros_like(hi)], axis=0).astype(BF16)
        for j in range(width // 128):
            cut = slice(j * 128, (j + 1) * 128)
            base = pl.multiple_of(2 * i * width + 256 * j, 256)
            lhs[:, pl.ds(base, 128)] = left[:, cut]
            lhs[:, pl.ds(base + 128, 128)] = right[:, cut]
        return total + value, area_total + a

    early = blocks - blocks // PARTS

    def pair(j, carry):
        left = lhs[:, pl.ds(pl.multiple_of(j * 256, 256), 256)]
        right = []
        for t in range(slots):
            weights = tiles[pl.ds(2 * j, 2), t].reshape(2 * block_cells, air_cells)
            hi, lo = split(weights)
            right.append(jnp.concatenate([hi, lo], axis=0))
        r = jnp.dot(left, jnp.concatenate(right, axis=1), preferred_element_type=F32)
        r = r[: 2 * fields] + r[2 * fields :]
        for t in range(slots):
            base = pl.multiple_of((t * carry[1] + carry[0] + 2 * j) * fields, 2 * fields)
            for q in range(lane_tiles):
                n = t * lane_tiles + q
                contrib[q, pl.ds(base, 2 * fields), :] = r[:, n * 128 : (n + 1) * 128]
        return carry

    def select(low, count):
        for t in range(slots):
            picks[:, pl.ds(2 * low + t * count, count)] = targets[pl.ds(t, 1), pl.ds(low, count)]
        tile_ids = picks[:, pl.ds(2 * low, slots * count)]
        owner_ids = lax.broadcasted_iota(jnp.int32, (owners, slots * count), 0)
        return jnp.where(owner_ids == tile_ids, 1.0, 0.0).astype(BF16)

    def collect(low, count, selector, g):
        right = []
        for f in (2 * g, 2 * g + 1):
            for q in range(lane_tiles):
                rows = pl.ds(slots * low * fields + f, slots * count, stride=fields)
                right.append(split(contrib[q, rows, :]))
        his = jnp.concatenate([r[0] for r in right], axis=1)
        los = jnp.concatenate([r[1] for r in right], axis=1)
        s = jnp.dot(selector, his, preferred_element_type=F32)
        s = s + jnp.dot(selector, los, preferred_element_type=F32)
        return [s[:, n * air_cells : (n + 1) * air_cells] for n in range(2)]

    def row_copy(p, slot):
        return pltpu.make_async_remote_copy(
            src_ref=row_out,
            dst_ref=rows_in.at[pl.ds(pl.multiple_of(slot * 8, 8), groups * lane_tiles)],
            send_sem=row_send,
            recv_sem=row_recv,
            device_id=(comp, p),
            device_id_type=MESH,
        )

    totals = (jnp.zeros((fields, width), F32), jnp.zeros((1, width), F32))
    weigh_rounds = flux_width // width
    low = 0
    arrived = 0
    step = 0
    for i in range(PARTS):
        flux_copies[i].wait()
        if i + 2 < PARTS:
            flux_copies[i + 2].start()
        if i == 1:
            for copy in small[3:]:
                copy.start()
        totals = lax.fori_loop(
            i * weigh_rounds, (i + 1) * weigh_rounds, weigh, totals, unroll=weigh_rounds
        )
        for size in round_plan[i]:
            if step == SEND_ROWS_AT:
                small[0].wait()
                for c in range(groups):
                    for q in range(lane_tiles):
                        row = fraction[pl.ds(c, 1), pl.ds(q * 128, 128)]
                        row_out[pl.ds(c * lane_tiles + q, 1), :] = row
                        rows_in[pl.ds(dom * 8 + c * lane_tiles + q, 1), :] = row
                start_more(EXTRA)
                pl.semaphore_wait(barrier, owners - 1)
                for c, p in rivals:
                    row_copy(p, dom).start()
            step += 1
            while arrived < len(tile_copies) and tile_copies[arrived][0] <= low + size:
                tile_copies[arrived][1].wait()
                start_more(1)
                arrived += 1
            first_block, count = (0, early) if low < early else (early, blocks - early)
            place = (slots * first_block - first_block, count)
            pairs = size // 2
            lax.fori_loop(
                low // 2,
                low // 2 + pairs,
                lambda j, c, place=place: (pair(j, place), c)[1],
                0,
                unroll=min(UNROLL, pairs),
            )
            low += size
        if low == early:
            small[3].wait()
            selector = select(0, early)
            last_selector = select(early, blocks - early)
            for g in range(fields // 2):
                summed[2 * g], summed[2 * g + 1] = collect(0, early, selector, g)

    far = pl.ds(pl.multiple_of(other * domains, 8), domains)
    own = pl.ds(pl.multiple_of(comp * domains, 8), domains)
    per_cut = fields // PAIR_CUTS
    pair_copies = []
    last = []
    for g in range(fields // 2):
        last.extend(collect(early, blocks - early, last_selector, g))
    for n in range(PAIR_CUTS):
        for f in range(n * per_cut, (n + 1) * per_cut):
            summed[f] = summed[f] + last[f]
        part = pl.ds(n * per_cut, per_cut)
        copy = pltpu.make_async_remote_copy(
            src_ref=summed.at[part, far],
            dst_ref=partner_in.at[part],
            send_sem=pair_send.at[n],
            recv_sem=pair_recv.at[n],
            device_id=(other, dom),
            device_id_type=MESH,
        )
        copy.start()
        pair_copies.append(copy)

    surface_num = jnp.sum(totals[0], axis=1, keepdims=True)
    surface_den = jnp.sum(totals[1])
    small[4].wait()
    small[5].wait()
    air_row = air[...].reshape(1, air_cells)
    inverse = 1.0 / air_row
    ocean_part = fraction[pl.ds(2, 1), :] * ocean[...]
    wet = air_row * ocean_part
    wet = sum(wet[:, q * 128 : (q + 1) * 128] for q in range(lane_tiles))
    air_den = jnp.sum(air_row)
    spot = lax.broadcasted_iota(jnp.int32, (fields, 128), 1)
    line = lax.broadcasted_iota(jnp.int32, (fields, 128), 0)
    stat = jnp.where(spot == line + 16 * comp, surface_num, 0.0)
    stat = jnp.sum(stat, axis=0, keepdims=True)
    spot1 = lax.broadcasted_iota(jnp.int32, (1, 128), 1)
    lead = spot1 - 64
    stat = stat + jnp.where((lead >= 16 * comp) & (lead < 16 * comp + 16), surface_den, 0.0)
    stat = stat + jnp.where(
        (lead >= 16 * groups) & (lead < 16 * groups + 16), air_den, 0.0
    )

    pltpu.make_async_remote_copy(
        src_ref=rows_in.at[pl.ds(0, (domains - 1) * groups * lane_tiles)],
        dst_ref=rows_in.at[pl.ds(0, (domains - 1) * groups * lane_tiles)],
        send_sem=row_send,
        recv_sem=row_recv,
        device_id=(other, dom),
        device_id_type=MESH,
    ).wait_recv()

    def shares(c):
        return [
            rows_in[pl.ds(c * lane_tiles + q, domains, stride=8), :]
            for q in range(lane_tiles)
        ]

    share_own = shares(comp)
    share_other = shares(other)

    half = domains // 2
    side = dom // half
    seat = dom % half
    bit = 1 + comp
    flip = dom // bit % 2
    neighbour = dom + bit * (1 - 2 * flip)

    def across(m, value):
        one = 2 * m + value
        two = m // 2 * 4 + 2 * value + m % 2
        return (1 - side) * half + one + comp * (two - one)

    rank = seat // 2 + comp * (seat // 4 * 2 + seat % 2 - seat // 2)
    mates_here = [side * half + k + jnp.where(seat <= k, 1, 0) for k in range(half - 1)]

    def message(src, dst, p, sem):
        return pltpu.make_async_remote_copy(
            src_ref=src.at[pl.ds(0, body_rows + 1)],
            dst_ref=dst.at[pl.ds(0, body_rows + 1)],
            send_sem=main_send,
            recv_sem=main_recv.at[sem],
            device_id=(comp, p),
            device_id_type=MESH,
        )

    def relay_copy(m):
        return message(
            outgoing.at[across(m, 1 - flip)], relayed.at[m], neighbour, domains + m
        )

    def direct_copy(p, slot):
        return message(outgoing.at[p], incoming.at[slot], p, slot)

    def stat_copy(p, slot):
        return pltpu.make_async_remote_copy(
            src_ref=stat_out,
            dst_ref=stat_in.at[slot],
            send_sem=stat_send,
            recv_sem=stat_recv,
            device_id=(other, p),
            device_id_type=MESH,
        )

    for n in range(PAIR_CUTS):
        pair_copies[n].wait_recv()
        for f in range(n * per_cut, (n + 1) * per_cut):
            acc = None
            for q in range(lane_tiles):
                cut = pl.ds(q * 128, 128)
                both = share_own[q] * summed[f, own, cut]
                both = both + share_other[q] * partner_in[f, :, cut]
                outgoing[:, q * fields + f, :] = both
                acc = both if acc is None else acc + both
            air_parts[pl.ds(f, 1), :] = jnp.sum(acc, axis=0, keepdims=True)
    air_num = jnp.sum(air_parts[...] + wet, axis=1, keepdims=True)
    air_num = jnp.where(spot == line + 16 * groups, air_num, 0.0)
    stat = stat + jnp.sum(air_num, axis=0, keepdims=True)
    outgoing[:, body_rows, :] = jnp.broadcast_to(stat, (domains, 128))
    stat_out[...] = stat
    for m in range(AT_ONCE):
        for value in range(2):
            group = jnp.where(flip == value, 0, half // 2)
            direct_copy(across(m, value), half + rank + group).start()
    for m in range(AT_ONCE, half // 2):
        relay_copy(m).start()
    for k in range(domains):
        stat_copy(k, dom).start()
    for m in range(AT_ONCE, half // 2):
        if m == SIDE_AT:
            for p in mates_here:
                direct_copy(p, seat).start()
        relay_copy(m).wait_recv()
        p = across(m, flip)
        outgoing[p] = outgoing[p] + relayed[m]
        direct_copy(p, half + rank).start()

    @pl.when(rank < AT_ONCE)
    def _():
        for m in range(half // 2):
            slot = half + half // 2 + m
            direct_copy(dom, slot).wait_recv()
            outgoing[dom] = outgoing[dom] + incoming[slot]

    stat = outgoing[dom, pl.ds(body_rows, 1), :]
    sums = []
    for q in range(lane_tiles):
        sums.append(outgoing[dom, pl.ds(q * fields, fields), :])
    slots_in = [p % half for p in mates_here] + [half + m for m in range(half // 2)]
    for slot in slots_in:
        direct_copy(dom, slot).wait_recv()
        for q in range(lane_tiles):
            sums[q] = sums[q] + incoming[slot, pl.ds(q * fields, fields), :]
        stat = stat + incoming[slot, pl.ds(body_rows, 1), :]
    for q in range(lane_tiles):
        cut = slice(q * 128, (q + 1) * 128)
        merged_ref[:, cut] = sums[q] * inverse[:, cut] + ocean_part[:, cut]

    pltpu.make_async_remote_copy(
        src_ref=stat_in,
        dst_ref=stat_in,
        send_sem=stat_send,
        recv_sem=stat_recv,
        device_id=(other, dom),
        device_id_type=MESH,
    ).wait_recv()
    stat = stat + jnp.sum(stat_in[...], axis=0)
    mean = stat / pltpu.roll(stat, 64, 1)
    for c in range(groups + 1):
        moved = mean if c == 0 else pltpu.roll(mean, 128 - 16 * c, 1)
        means_ref[pl.ds(c, 1), :] = moved[:, :fields]

    pltpu.make_async_remote_copy(
        src_ref=rows_in.at[pl.ds(0, (domains - 1) * groups * lane_tiles)],
        dst_ref=rows_in.at[pl.ds(0, (domains - 1) * groups * lane_tiles)],
        send_sem=row_send,
        recv_sem=row_recv,
        device_id=(other, dom),
        device_id_type=MESH,
    ).wait_send()
    for copy in pair_copies:
        copy.wait_send()
    pltpu.make_async_remote_copy(
        src_ref=stat_in,
        dst_ref=stat_in,
        send_sem=stat_send,
        recv_sem=stat_recv,
        device_id=(other, dom),
        device_id_type=MESH,
    ).wait_send()
    pltpu.make_async_remote_copy(
        src_ref=outgoing.at[pl.ds(0, domains - 1), pl.ds(0, body_rows + 1)],
        dst_ref=outgoing.at[pl.ds(0, domains - 1), pl.ds(0, body_rows + 1)],
        send_sem=main_send,
        recv_sem=main_recv.at[0],
        device_id=(other, dom),
        device_id_type=MESH,
    ).wait_send()


def finish(merged_in, means_in, merged_ref, means_ref):
    merged_ref[...] = merged_in[...]
    means_ref[...] = means_in[...]


def on_device(
    surface_flux,
    active_mask,
    source_area,
    tile_targets,
    remap_tiles,
    ocean_flux,
    air_fraction,
    air_area,
):
    groups = lax.axis_size("comp")
    domains = lax.axis_size("dom")
    owners = groups * domains
    fields = surface_flux.shape[1]
    cells = surface_flux.shape[2]
    blocks, slots, block_cells, air_cells = remap_tiles.shape
    lane_tiles = air_cells // 128
    message = -(-(lane_tiles * fields + 1) // 8) * 8
    vmem = pl.BlockSpec(memory_space=pltpu.VMEM)
    hbm = pl.BlockSpec(memory_space=pltpu.HBM)
    dma = pltpu.SemaphoreType.DMA
    parts = pl.pallas_call(
        functools.partial(kernel, groups, domains),
        out_shape=(
            pltpu.VMEM((fields, air_cells), F32),
            pltpu.VMEM((groups + 1, fields), F32),
        ),
        in_specs=[hbm] * 8,
        out_specs=(vmem, vmem),
        scratch_shapes=[
            pltpu.VMEM(surface_flux.shape, F32),
            pltpu.VMEM((1, cells), jnp.int32),
            pltpu.VMEM((1, cells), F32),
            pltpu.VMEM((slots, blocks), jnp.int32),
            pltpu.VMEM(remap_tiles.shape, F32),
            pltpu.VMEM(ocean_flux.shape, F32),
            pltpu.VMEM(air_fraction.shape, F32),
            pltpu.VMEM((air_cells,), F32),
            pltpu.VMEM((2 * fields, cells), F32),
            pltpu.VMEM((4 * fields, 2 * cells), BF16),
            pltpu.VMEM((lane_tiles, blocks * slots * fields, 128), F32),
            pltpu.VMEM((1, blocks * slots), jnp.int32),
            pltpu.VMEM((groups * lane_tiles, 128), F32),
            pltpu.VMEM((domains * 8, 128), F32),
            pltpu.VMEM((fields, owners, air_cells), F32),
            pltpu.VMEM((fields, 128), F32),
            pltpu.VMEM((fields, domains, air_cells), F32),
            pltpu.VMEM((1, 128), F32),
            pltpu.VMEM((domains, 1, 128), F32),
            pltpu.VMEM((domains, message, 128), F32),
            pltpu.VMEM((domains, message, 128), F32),
            pltpu.VMEM((domains // 4, message, 128), F32),
            dma((PARTS,)),
            dma((sum(len(c) for c in plan(blocks)[0]),)),
            dma((6,)),
            dma,
            dma,
            dma((PAIR_CUTS,)),
            dma((PAIR_CUTS,)),
            dma,
            dma,
            dma,
            dma((domains + domains // 4,)),
        ],
        compiler_params=pltpu.CompilerParams(
            collective_id=0, has_side_effects=True, vmem_limit_bytes=60 * 1024 * 1024
        ),
    )(
        surface_flux,
        active_mask.reshape(1, cells),
        source_area.reshape(1, cells),
        tile_targets.T,
        remap_tiles,
        ocean_flux,
        air_fraction,
        air_area,
    )
    return pl.pallas_call(
        finish,
        out_shape=(
            jax.ShapeDtypeStruct((fields, air_cells), F32),
            jax.ShapeDtypeStruct((groups + 1, fields), F32),
        ),
        in_specs=[vmem, vmem],
        out_specs=(vmem, vmem),
    )(*[pltpu.with_memory_space_constraint(p, pltpu.VMEM) for p in parts])


def solution(mesh):
    in_specs = (
        P(None, None, ("comp", "dom")),
        P(("comp", "dom")),
        P(("comp", "dom")),
        P(("comp", "dom"), None),
        P(("comp", "dom"), None, None, None),
        P(None, ("comp", "dom")),
        P(None, ("comp", "dom")),
        P(("comp", "dom")),
    )
    out_specs = (P(None, ("comp", "dom")), P())
    return jax.shard_map(
        on_device, mesh=mesh, in_specs=in_specs, out_specs=out_specs, check_vma=False
    )
```

```python
import functools

import jax
import jax.numpy as jnp
from jax import lax
from jax.experimental import pallas as pl
from jax.experimental.pallas import tpu as pltpu
from jax.sharding import PartitionSpec as P

MESH = pl.DeviceIdType.MESH
F32 = jnp.float32
BF16 = jnp.bfloat16
DEPTH = 12
EXTRA = 4
TURNS = (1, 2, 3)
PARTS = 4
UNROLL = 8
PAIR_CUTS = 3
SIDE_AT = 3


def split(x):
    hi = x.astype(BF16)
    lo = (x - hi.astype(F32)).astype(BF16)
    return hi, lo


def plan(blocks):
    whole = blocks // PARTS
    copies = [[whole // 4] * 4] * PARTS
    rounds = [[whole // 2] * 2] + [[whole]] * (PARTS - 2) + [[whole // 2, whole // 4, whole // 4]]
    return copies, rounds


def kernel(
    groups,
    domains,
    flux_hbm,
    mask_hbm,
    area_hbm,
    targets_hbm,
    tiles_hbm,
    ocean_hbm,
    fraction_hbm,
    air_hbm,
    merged_ref,
    means_ref,
    flux,
    mask,
    area,
    targets,
    tiles,
    ocean,
    fraction,
    air,
    stacked,
    lhs,
    contrib,
    picks,
    row_out,
    rows_in,
    summed,
    air_parts,
    partner_in,
    stat_out,
    stat_in,
    outgoing,
    incoming,
    relayed,
    flux_sem,
    tile_sem,
    small_sem,
    row_send,
    row_recv,
    pair_send,
    pair_recv,
    stat_send,
    stat_recv,
    main_send,
    main_recv,
):
    steps, fields, cells = flux.shape
    blocks, slots, block_cells, air_cells = tiles.shape
    owners = groups * domains
    copy_plan, round_plan = plan(blocks)
    lane_tiles = air_cells // 128
    body_rows = lane_tiles * fields
    comp = lax.axis_index("comp")
    dom = lax.axis_index("dom")
    other = 1 - comp

    small = [
        pltpu.make_async_copy(src, dst, small_sem.at[i])
        for i, (src, dst) in enumerate(
            [
                (fraction_hbm, fraction),
                (mask_hbm, mask),
                (area_hbm, area),
                (targets_hbm, targets),
                (ocean_hbm, ocean),
                (air_hbm, air),
            ]
        )
    ]
    for copy in small[1:3]:
        copy.start()
    flux_width = cells // PARTS
    flux_copies = []
    tile_copies = []
    waiting = []
    low = 0
    for i in range(PARTS):
        part = pl.ds(i * flux_width, flux_width)
        flux_copies.append(
            pltpu.make_async_copy(flux_hbm.at[:, :, part], flux.at[:, :, part], flux_sem.at[i])
        )
        for size in copy_plan[i]:
            part = pl.ds(low, size)
            low += size
            copy = pltpu.make_async_copy(
                tiles_hbm.at[part], tiles.at[part], tile_sem.at[len(tile_copies)]
            )
            tile_copies.append((low, copy))
            waiting.append(copy)

    def start_more(count):
        for copy in waiting[:count]:
            copy.start(priority=1)
        del waiting[:count]

    for copy in flux_copies:
        copy.start()
    start_more(DEPTH)
    small[0].start()

    barrier = pltpu.get_barrier_semaphore()
    rivals = []
    for k in range(domains - 1):
        rivals.append((comp, k + jnp.where(dom <= k, 1, 0)))
    mates = [(other, k) for k in range(domains)]
    for a, b in zip(rivals + [None], mates):
        for peer in (a, b):
            if peer is not None:
                pl.semaphore_signal(barrier, inc=1, device_id=peer, device_id_type=MESH)

    small[1].wait()
    small[2].wait()
    width = min(512, flux_width)
    lane = lax.broadcasted_iota(jnp.int32, (fields, width), 1)
    first = lax.rem(lane, 2 * block_cells) < block_cells

    def weigh(i, carry):
        total, area_total = carry
        part = pl.ds(pl.multiple_of(i * width, width), width)
        value = flux[0, :, part]
        for s in range(1, steps):
            value = value + flux[s, :, part]
        a = area[:, part]
        value = (value / steps) * (mask[:, part].astype(F32) * a)
        stacked[pl.ds(0, fields), part] = jnp.where(first, value, 0.0)
        stacked[pl.ds(fields, fields), part] = jnp.where(first, 0.0, value)
        both = stacked[:, part]
        hi = both.astype(BF16).astype(F32)
        left = jnp.concatenate([hi, both - hi], axis=0).astype(BF16)
        right = jnp.concatenate([hi, jnp.zeros_like(hi)], axis=0).astype(BF16)
        for j in range(width // 128):
            cut = slice(j * 128, (j + 1) * 128)
            base = pl.multiple_of(2 * i * width + 256 * j, 256)
            lhs[:, pl.ds(base, 128)] = left[:, cut]
            lhs[:, pl.ds(base + 128, 128)] = right[:, cut]
        return total + value, area_total + a

    early = blocks - blocks // PARTS

    def pair(j, carry):
        left = lhs[:, pl.ds(pl.multiple_of(j * 256, 256), 256)]
        right = []
        for t in range(slots):
            weights = tiles[pl.ds(2 * j, 2), t].reshape(2 * block_cells, air_cells)
            hi, lo = split(weights)
            right.append(jnp.concatenate([hi, lo], axis=0))
        r = jnp.dot(left, jnp.concatenate(right, axis=1), preferred_element_type=F32)
        r = r[: 2 * fields] + r[2 * fields :]
        for t in range(slots):
            base = pl.multiple_of((t * carry[1] + carry[0] + 2 * j) * fields, 2 * fields)
            for q in range(lane_tiles):
                n = t * lane_tiles + q
                contrib[q, pl.ds(base, 2 * fields), :] = r[:, n * 128 : (n + 1) * 128]
        return carry

    def select(low, count):
        for t in range(slots):
            picks[:, pl.ds(2 * low + t * count, count)] = targets[pl.ds(t, 1), pl.ds(low, count)]
        tile_ids = picks[:, pl.ds(2 * low, slots * count)]
        owner_ids = lax.broadcasted_iota(jnp.int32, (owners, slots * count), 0)
        return jnp.where(owner_ids == tile_ids, 1.0, 0.0).astype(BF16)

    def collect(low, count, selector, g):
        right = []
        for f in (2 * g, 2 * g + 1):
            for q in range(lane_tiles):
                rows = pl.ds(slots * low * fields + f, slots * count, stride=fields)
                right.append(split(contrib[q, rows, :]))
        his = jnp.concatenate([r[0] for r in right], axis=1)
        los = jnp.concatenate([r[1] for r in right], axis=1)
        s = jnp.dot(selector, his, preferred_element_type=F32)
        s = s + jnp.dot(selector, los, preferred_element_type=F32)
        return [s[:, n * air_cells : (n + 1) * air_cells] for n in range(2)]

    def row_copy(p, slot):
        return pltpu.make_async_remote_copy(
            src_ref=row_out,
            dst_ref=rows_in.at[pl.ds(pl.multiple_of(slot * 8, 8), groups * lane_tiles)],
            send_sem=row_send,
            recv_sem=row_recv,
            device_id=(comp, p),
            device_id_type=MESH,
        )

    def send_rows():
        small[0].wait()
        for c in range(groups):
            for q in range(lane_tiles):
                row = fraction[pl.ds(c, 1), pl.ds(q * 128, 128)]
                row_out[pl.ds(c * lane_tiles + q, 1), :] = row
                rows_in[pl.ds(dom * 8 + c * lane_tiles + q, 1), :] = row
        pl.semaphore_wait(barrier, owners - 1)
        for c, p in rivals:
            row_copy(p, dom).start()

    quarter = domains // 4
    turns = [
        (TURNS[0], (3 * quarter, domains)),
        (TURNS[1], (2 * quarter, 3 * quarter)),
        (TURNS[2], (1, 2 * quarter)),
    ]

    totals = (jnp.zeros((fields, width), F32), jnp.zeros((1, width), F32))
    weigh_rounds = flux_width // width
    low = 0
    arrived = 0
    step = 0
    for i in range(PARTS):
        flux_copies[i].wait()
        if i == 1:
            for copy in small[3:]:
                copy.start()
        totals = lax.fori_loop(
            i * weigh_rounds, (i + 1) * weigh_rounds, weigh, totals, unroll=weigh_rounds
        )
        for size in round_plan[i]:
            for low_dom, high_dom in [span for at, span in turns if at == step]:
                pl.when((dom >= low_dom) & (dom < high_dom))(send_rows)
            step += 1
            while arrived < len(tile_copies) and tile_copies[arrived][0] <= low + size:
                tile_copies[arrived][1].wait()
                start_more(1)
                arrived += 1
            first_block, count = (0, early) if low < early else (early, blocks - early)
            place = (slots * first_block - first_block, count)
            pairs = size // 2
            lax.fori_loop(
                low // 2,
                low // 2 + pairs,
                lambda j, c, place=place: (pair(j, place), c)[1],
                0,
                unroll=min(UNROLL, pairs),
            )
            low += size
        if low == early:
            small[3].wait()
            selector = select(0, early)
            last_selector = select(early, blocks - early)
            for g in range(fields // 2):
                summed[2 * g], summed[2 * g + 1] = collect(0, early, selector, g)

    pl.when(dom == 0)(send_rows)

    far = pl.ds(pl.multiple_of(other * domains, 8), domains)
    own = pl.ds(pl.multiple_of(comp * domains, 8), domains)
    per_cut = fields // PAIR_CUTS
    pair_copies = []
    last = []
    for g in range(fields // 2):
        last.extend(collect(early, blocks - early, last_selector, g))
    for n in range(PAIR_CUTS):
        for f in range(n * per_cut, (n + 1) * per_cut):
            summed[f] = summed[f] + last[f]
        part = pl.ds(n * per_cut, per_cut)
        copy = pltpu.make_async_remote_copy(
            src_ref=summed.at[part, far],
            dst_ref=partner_in.at[part],
            send_sem=pair_send.at[n],
            recv_sem=pair_recv.at[n],
            device_id=(other, dom),
            device_id_type=MESH,
        )
        copy.start()
        pair_copies.append(copy)

    surface_num = jnp.sum(totals[0], axis=1, keepdims=True)
    surface_den = jnp.sum(totals[1])
    small[4].wait()
    small[5].wait()
    air_row = air[...].reshape(1, air_cells)
    inverse = 1.0 / air_row
    ocean_part = fraction[pl.ds(2, 1), :] * ocean[...]
    wet = air_row * ocean_part
    wet = sum(wet[:, q * 128 : (q + 1) * 128] for q in range(lane_tiles))
    air_den = jnp.sum(air_row)
    spot = lax.broadcasted_iota(jnp.int32, (fields, 128), 1)
    line = lax.broadcasted_iota(jnp.int32, (fields, 128), 0)
    stat = jnp.where(spot == line + 16 * comp, surface_num, 0.0)
    stat = jnp.sum(stat, axis=0, keepdims=True)
    spot1 = lax.broadcasted_iota(jnp.int32, (1, 128), 1)
    lead = spot1 - 64
    stat = stat + jnp.where((lead >= 16 * comp) & (lead < 16 * comp + 16), surface_den, 0.0)
    stat = stat + jnp.where(
        (lead >= 16 * groups) & (lead < 16 * groups + 16), air_den, 0.0
    )

    pltpu.make_async_remote_copy(
        src_ref=rows_in.at[pl.ds(0, (domains - 1) * groups * lane_tiles)],
        dst_ref=rows_in.at[pl.ds(0, (domains - 1) * groups * lane_tiles)],
        send_sem=row_send,
        recv_sem=row_recv,
        device_id=(other, dom),
        device_id_type=MESH,
    ).wait_recv()

    def shares(c):
        return [
            rows_in[pl.ds(c * lane_tiles + q, domains, stride=8), :]
            for q in range(lane_tiles)
        ]

    share_own = shares(comp)
    share_other = shares(other)

    half = domains // 2
    side = dom // half
    seat = dom % half
    bit = 1 + comp
    flip = dom // bit % 2
    neighbour = dom + bit * (1 - 2 * flip)

    def across(m, value):
        one = 2 * m + value
        two = m // 2 * 4 + 2 * value + m % 2
        return (1 - side) * half + one + comp * (two - one)

    rank = seat // 2 + comp * (seat // 4 * 2 + seat % 2 - seat // 2)
    mates_here = [side * half + k + jnp.where(seat <= k, 1, 0) for k in range(half - 1)]

    def message(src, dst, p, sem):
        return pltpu.make_async_remote_copy(
            src_ref=src.at[pl.ds(0, body_rows + 1)],
            dst_ref=dst.at[pl.ds(0, body_rows + 1)],
            send_sem=main_send,
            recv_sem=main_recv.at[sem],
            device_id=(comp, p),
            device_id_type=MESH,
        )

    def relay_copy(m):
        return message(
            outgoing.at[across(m, 1 - flip)], relayed.at[m], neighbour, domains + m
        )

    def direct_copy(p, slot):
        return message(outgoing.at[p], incoming.at[slot], p, slot)

    def stat_copy(p, slot):
        return pltpu.make_async_remote_copy(
            src_ref=stat_out,
            dst_ref=stat_in.at[slot],
            send_sem=stat_send,
            recv_sem=stat_recv,
            device_id=(other, p),
            device_id_type=MESH,
        )

    for n in range(PAIR_CUTS):
        pair_copies[n].wait_recv()
        for f in range(n * per_cut, (n + 1) * per_cut):
            acc = None
            for q in range(lane_tiles):
                cut = pl.ds(q * 128, 128)
                both = share_own[q] * summed[f, own, cut]
                both = both + share_other[q] * partner_in[f, :, cut]
                outgoing[:, q * fields + f, :] = both
                acc = both if acc is None else acc + both
            air_parts[pl.ds(f, 1), :] = jnp.sum(acc, axis=0, keepdims=True)
    air_num = jnp.sum(air_parts[...] + wet, axis=1, keepdims=True)
    air_num = jnp.where(spot == line + 16 * groups, air_num, 0.0)
    stat = stat + jnp.sum(air_num, axis=0, keepdims=True)
    outgoing[:, body_rows, :] = jnp.broadcast_to(stat, (domains, 128))
    stat_out[...] = stat
    def at_once(target):
        return (dom >= 2 * quarter) & (target == 0)

    for m in range(half // 2):
        target = across(m, 1 - flip)

        @pl.when(at_once(target))
        def _(target=target):
            direct_copy(target, domains - half // 2 + rank).start()

        @pl.when(jnp.logical_not(at_once(target)))
        def _(m=m):
            relay_copy(m).start()

    direct_copy(mates_here[0], seat).start()
    for k in range(domains):
        stat_copy(k, dom).start()
    for m in range(half // 2):
        if m == SIDE_AT:
            for p in mates_here[1:]:
                direct_copy(p, seat).start()
        target = across(m, flip)

        @pl.when(jnp.logical_not(at_once(target)))
        def _(m=m, target=target):
            relay_copy(m).wait_recv()
            outgoing[target] = outgoing[target] + relayed[m]

        direct_copy(target, half + rank).start()

    @pl.when(dom == 0)
    def _():
        for m in range(half // 2):
            slot = domains - half // 2 + m
            direct_copy(dom, slot).wait_recv()
            outgoing[dom] = outgoing[dom] + incoming[slot]

    stat = outgoing[dom, pl.ds(body_rows, 1), :]
    sums = []
    for q in range(lane_tiles):
        sums.append(outgoing[dom, pl.ds(q * fields, fields), :])
    slots_in = [p % half for p in mates_here] + [half + m for m in range(half // 2)]
    for slot in slots_in:
        direct_copy(dom, slot).wait_recv()
        for q in range(lane_tiles):
            sums[q] = sums[q] + incoming[slot, pl.ds(q * fields, fields), :]
        stat = stat + incoming[slot, pl.ds(body_rows, 1), :]
    for q in range(lane_tiles):
        cut = slice(q * 128, (q + 1) * 128)
        merged_ref[:, cut] = sums[q] * inverse[:, cut] + ocean_part[:, cut]

    pltpu.make_async_remote_copy(
        src_ref=stat_in,
        dst_ref=stat_in,
        send_sem=stat_send,
        recv_sem=stat_recv,
        device_id=(other, dom),
        device_id_type=MESH,
    ).wait_recv()
    stat = stat + jnp.sum(stat_in[...], axis=0)
    mean = stat / pltpu.roll(stat, 64, 1)
    for c in range(groups + 1):
        moved = mean if c == 0 else pltpu.roll(mean, 128 - 16 * c, 1)
        means_ref[pl.ds(c, 1), :] = moved[:, :fields]

    pltpu.make_async_remote_copy(
        src_ref=rows_in.at[pl.ds(0, (domains - 1) * groups * lane_tiles)],
        dst_ref=rows_in.at[pl.ds(0, (domains - 1) * groups * lane_tiles)],
        send_sem=row_send,
        recv_sem=row_recv,
        device_id=(other, dom),
        device_id_type=MESH,
    ).wait_send()
    for copy in pair_copies:
        copy.wait_send()
    pltpu.make_async_remote_copy(
        src_ref=stat_in,
        dst_ref=stat_in,
        send_sem=stat_send,
        recv_sem=stat_recv,
        device_id=(other, dom),
        device_id_type=MESH,
    ).wait_send()
    pltpu.make_async_remote_copy(
        src_ref=outgoing.at[pl.ds(0, domains - 1), pl.ds(0, body_rows + 1)],
        dst_ref=outgoing.at[pl.ds(0, domains - 1), pl.ds(0, body_rows + 1)],
        send_sem=main_send,
        recv_sem=main_recv.at[0],
        device_id=(other, dom),
        device_id_type=MESH,
    ).wait_send()


def finish(merged_in, means_in, merged_ref, means_ref):
    merged_ref[...] = merged_in[...]
    means_ref[...] = means_in[...]


def on_device(
    surface_flux,
    active_mask,
    source_area,
    tile_targets,
    remap_tiles,
    ocean_flux,
    air_fraction,
    air_area,
):
    groups = lax.axis_size("comp")
    domains = lax.axis_size("dom")
    owners = groups * domains
    fields = surface_flux.shape[1]
    cells = surface_flux.shape[2]
    blocks, slots, block_cells, air_cells = remap_tiles.shape
    lane_tiles = air_cells // 128
    message = -(-(lane_tiles * fields + 1) // 8) * 8
    vmem = pl.BlockSpec(memory_space=pltpu.VMEM)
    hbm = pl.BlockSpec(memory_space=pltpu.HBM)
    dma = pltpu.SemaphoreType.DMA
    parts = pl.pallas_call(
        functools.partial(kernel, groups, domains),
        out_shape=(
            pltpu.VMEM((fields, air_cells), F32),
            pltpu.VMEM((groups + 1, fields), F32),
        ),
        in_specs=[hbm] * 8,
        out_specs=(vmem, vmem),
        scratch_shapes=[
            pltpu.VMEM(surface_flux.shape, F32),
            pltpu.VMEM((1, cells), jnp.int32),
            pltpu.VMEM((1, cells), F32),
            pltpu.VMEM((slots, blocks), jnp.int32),
            pltpu.VMEM(remap_tiles.shape, F32),
            pltpu.VMEM(ocean_flux.shape, F32),
            pltpu.VMEM(air_fraction.shape, F32),
            pltpu.VMEM((air_cells,), F32),
            pltpu.VMEM((2 * fields, cells), F32),
            pltpu.VMEM((4 * fields, 2 * cells), BF16),
            pltpu.VMEM((lane_tiles, blocks * slots * fields, 128), F32),
            pltpu.VMEM((1, blocks * slots), jnp.int32),
            pltpu.VMEM((groups * lane_tiles, 128), F32),
            pltpu.VMEM((domains * 8, 128), F32),
            pltpu.VMEM((fields, owners, air_cells), F32),
            pltpu.VMEM((fields, 128), F32),
            pltpu.VMEM((fields, domains, air_cells), F32),
            pltpu.VMEM((1, 128), F32),
            pltpu.VMEM((domains, 1, 128), F32),
            pltpu.VMEM((domains, message, 128), F32),
            pltpu.VMEM((domains, message, 128), F32),
            pltpu.VMEM((domains // 4, message, 128), F32),
            dma((PARTS,)),
            dma((sum(len(c) for c in plan(blocks)[0]),)),
            dma((6,)),
            dma,
            dma,
            dma((PAIR_CUTS,)),
            dma((PAIR_CUTS,)),
            dma,
            dma,
            dma,
            dma((domains + domains // 4,)),
        ],
        compiler_params=pltpu.CompilerParams(
            collective_id=0, has_side_effects=True, vmem_limit_bytes=60 * 1024 * 1024
        ),
    )(
        surface_flux,
        active_mask.reshape(1, cells),
        source_area.reshape(1, cells),
        tile_targets.T,
        remap_tiles,
        ocean_flux,
        air_fraction,
        air_area,
    )
    return pl.pallas_call(
        finish,
        out_shape=(
            jax.ShapeDtypeStruct((fields, air_cells), F32),
            jax.ShapeDtypeStruct((groups + 1, fields), F32),
        ),
        in_specs=[vmem, vmem],
        out_specs=(vmem, vmem),
    )(*[pltpu.with_memory_space_constraint(p, pltpu.VMEM) for p in parts])


def solution(mesh):
    in_specs = (
        P(None, None, ("comp", "dom")),
        P(("comp", "dom")),
        P(("comp", "dom")),
        P(("comp", "dom"), None),
        P(("comp", "dom"), None, None, None),
        P(None, ("comp", "dom")),
        P(None, ("comp", "dom")),
        P(("comp", "dom")),
    )
    out_specs = (P(None, ("comp", "dom")), P())
    return jax.shard_map(
        on_device, mesh=mesh, in_specs=in_specs, out_specs=out_specs, check_vma=False
    )
```

```python
import functools

import jax
import jax.numpy as jnp
from jax import lax
from jax.experimental import pallas as pl
from jax.experimental.pallas import tpu as pltpu
from jax.sharding import PartitionSpec as P

MESH = pl.DeviceIdType.MESH
F32 = jnp.float32
BF16 = jnp.bfloat16
DEPTH = 5
TURNS = (1, 2, 3)
PARTS = 4
UNROLL = 8
PAIR_CUTS = 3
SIDE_AT = (0, 99)


def split(x):
    hi = x.astype(BF16)
    lo = (x - hi.astype(F32)).astype(BF16)
    return hi, lo


def plan(blocks):
    whole = blocks // PARTS
    rounds = [[whole // 2] * 2] + [[whole]] * (PARTS - 2) + [[whole // 2, whole // 4, whole // 4]]
    return rounds, rounds


def kernel(
    groups,
    domains,
    flux_hbm,
    mask_hbm,
    area_hbm,
    targets_hbm,
    tiles_hbm,
    ocean_hbm,
    fraction_hbm,
    air_hbm,
    merged_ref,
    means_ref,
    flux,
    mask,
    area,
    targets,
    tiles,
    ocean,
    fraction,
    air,
    stacked,
    lhs,
    contrib,
    picks,
    row_out,
    rows_in,
    summed,
    air_parts,
    partner_in,
    stat_out,
    stat_in,
    outgoing,
    incoming,
    relayed,
    flux_sem,
    tile_sem,
    small_sem,
    row_send,
    row_recv,
    pair_send,
    pair_recv,
    stat_send,
    stat_recv,
    main_send,
    main_recv,
):
    steps, fields, cells = flux.shape
    blocks, slots, block_cells, air_cells = tiles.shape
    owners = groups * domains
    copy_plan, round_plan = plan(blocks)
    lane_tiles = air_cells // 128
    body_rows = lane_tiles * fields
    comp = lax.axis_index("comp")
    dom = lax.axis_index("dom")
    other = 1 - comp

    small = [
        pltpu.make_async_copy(src, dst, small_sem.at[i])
        for i, src, dst in (
            [
                (0, fraction_hbm, fraction),
                (1, mask_hbm, mask),
                (1, area_hbm, area),
                (2, targets_hbm, targets),
                (3, ocean_hbm, ocean),
                (4, air_hbm, air),
            ]
        )
    ]
    for copy in small[1:3]:
        copy.start()
    flux_width = cells // PARTS
    flux_copies = []
    tile_copies = []
    waiting = []
    low = 0
    for i in range(PARTS):
        part = pl.ds(i * flux_width, flux_width)
        flux_copies.append(
            pltpu.make_async_copy(flux_hbm.at[:, :, part], flux.at[:, :, part], flux_sem.at[i])
        )
        for size in copy_plan[i]:
            part = pl.ds(low, size)
            low += size
            copy = pltpu.make_async_copy(
                tiles_hbm.at[part], tiles.at[part], tile_sem.at[len(tile_copies)]
            )
            tile_copies.append((low, copy))
            waiting.append(copy)

    def start_more(count):
        for copy in waiting[:count]:
            copy.start(priority=1)
        del waiting[:count]

    for copy in flux_copies:
        copy.start()
    start_more(DEPTH)
    small[0].start()

    barrier = pltpu.get_barrier_semaphore()
    rivals = []
    for k in range(domains - 1):
        rivals.append((comp, k + jnp.where(dom <= k, 1, 0)))
    mates = [(other, k) for k in range(domains)]
    for a, b in zip(rivals + [None], mates):
        for peer in (a, b):
            if peer is not None:
                pl.semaphore_signal(barrier, inc=1, device_id=peer, device_id_type=MESH)

    both_rows = contrib.at[0, pl.ds(0, 2 * cells // 128)]
    pltpu.make_async_copy(both_rows, both_rows, small_sem.at[1]).wait()
    width = min(512, flux_width)
    lane = lax.broadcasted_iota(jnp.int32, (fields, width), 1)
    first = lax.rem(lane, 2 * block_cells) < block_cells

    def weigh(i, carry):
        total, area_total = carry
        part = pl.ds(pl.multiple_of(i * width, width), width)
        value = flux[0, :, part]
        for s in range(1, steps):
            value = value + flux[s, :, part]
        a = area[:, part]
        value = (value / steps) * (mask[:, part].astype(F32) * a)
        stacked[pl.ds(0, fields), part] = jnp.where(first, value, 0.0)
        stacked[pl.ds(fields, fields), part] = jnp.where(first, 0.0, value)
        both = stacked[:, part]
        hi = both.astype(BF16).astype(F32)
        left = jnp.concatenate([hi, both - hi], axis=0).astype(BF16)
        right = jnp.concatenate([hi, jnp.zeros_like(hi)], axis=0).astype(BF16)
        for j in range(width // 128):
            cut = slice(j * 128, (j + 1) * 128)
            base = pl.multiple_of(2 * i * width + 256 * j, 256)
            lhs[:, pl.ds(base, 128)] = left[:, cut]
            lhs[:, pl.ds(base + 128, 128)] = right[:, cut]
        return total + value, area_total + a

    early = blocks - blocks // PARTS

    def pair(j, carry):
        left = lhs[:, pl.ds(pl.multiple_of(j * 256, 256), 256)]
        right = []
        for t in range(slots):
            weights = tiles[pl.ds(2 * j, 2), t].reshape(2 * block_cells, air_cells)
            hi, lo = split(weights)
            right.append(jnp.concatenate([hi, lo], axis=0))
        r = jnp.dot(left, jnp.concatenate(right, axis=1), preferred_element_type=F32)
        r = r[: 2 * fields] + r[2 * fields :]
        for t in range(slots):
            base = pl.multiple_of((t * carry[1] + carry[0] + 2 * j) * fields, 2 * fields)
            for q in range(lane_tiles):
                n = t * lane_tiles + q
                contrib[q, pl.ds(base, 2 * fields), :] = r[:, n * 128 : (n + 1) * 128]
        return carry

    def select(low, count):
        for t in range(slots):
            picks[:, pl.ds(2 * low + t * count, count)] = targets[pl.ds(t, 1), pl.ds(low, count)]
        tile_ids = picks[:, pl.ds(2 * low, slots * count)]
        owner_ids = lax.broadcasted_iota(jnp.int32, (owners, slots * count), 0)
        return jnp.where(owner_ids == tile_ids, 1.0, 0.0).astype(BF16)

    def collect(low, count, selector, g):
        right = []
        for f in (2 * g, 2 * g + 1):
            for q in range(lane_tiles):
                rows = pl.ds(slots * low * fields + f, slots * count, stride=fields)
                right.append(split(contrib[q, rows, :]))
        his = jnp.concatenate([r[0] for r in right], axis=1)
        los = jnp.concatenate([r[1] for r in right], axis=1)
        s = jnp.dot(selector, his, preferred_element_type=F32)
        s = s + jnp.dot(selector, los, preferred_element_type=F32)
        return [s[:, n * air_cells : (n + 1) * air_cells] for n in range(2)]

    def row_copy(p, slot):
        return pltpu.make_async_remote_copy(
            src_ref=row_out,
            dst_ref=rows_in.at[pl.ds(pl.multiple_of(slot * 8, 8), groups * lane_tiles)],
            send_sem=row_send,
            recv_sem=row_recv,
            device_id=(comp, p),
            device_id_type=MESH,
        )

    def send_rows():
        small[0].wait()
        for c in range(groups):
            for q in range(lane_tiles):
                row = fraction[pl.ds(c, 1), pl.ds(q * 128, 128)]
                row_out[pl.ds(c * lane_tiles + q, 1), :] = row
                rows_in[pl.ds(dom * 8 + c * lane_tiles + q, 1), :] = row
        pl.semaphore_wait(barrier, owners - 1)
        for c, p in rivals:
            row_copy(p, dom).start()

    quarter = domains // 4
    turns = [
        (TURNS[0], (3 * quarter, domains)),
        (TURNS[1], (2 * quarter, 3 * quarter)),
        (TURNS[2], (1, 2 * quarter)),
    ]

    totals = (jnp.zeros((fields, width), F32), jnp.zeros((1, width), F32))
    weigh_rounds = flux_width // width
    low = 0
    arrived = 0
    step = 0
    for i in range(PARTS):
        flux_copies[i].wait()
        if i == 1:
            for copy in small[3:]:
                copy.start()
        totals = lax.fori_loop(
            i * weigh_rounds, (i + 1) * weigh_rounds, weigh, totals, unroll=weigh_rounds
        )
        for size in round_plan[i]:
            for low_dom, high_dom in [span for at, span in turns if at == step]:
                pl.when((dom >= low_dom) & (dom < high_dom))(send_rows)
            step += 1
            while arrived < len(tile_copies) and tile_copies[arrived][0] <= low + size:
                tile_copies[arrived][1].wait()
                start_more(1)
                arrived += 1
            first_block, count = (0, early) if low < early else (early, blocks - early)
            place = (slots * first_block - first_block, count)
            pairs = size // 2
            lax.fori_loop(
                low // 2,
                low // 2 + pairs,
                lambda j, c, place=place: (pair(j, place), c)[1],
                0,
                unroll=min(UNROLL, pairs),
            )
            low += size
        if low == early:
            small[3].wait()
            selector = select(0, early)
            last_selector = select(early, blocks - early)
            for g in range(fields // 2):
                summed[2 * g], summed[2 * g + 1] = collect(0, early, selector, g)

    pl.when(dom == 0)(send_rows)

    far = pl.ds(pl.multiple_of(other * domains, 8), domains)
    own = pl.ds(pl.multiple_of(comp * domains, 8), domains)
    per_cut = fields // PAIR_CUTS
    pair_copies = []
    last = []
    for g in range(fields // 2):
        last.extend(collect(early, blocks - early, last_selector, g))
    for n in range(PAIR_CUTS):
        for f in range(n * per_cut, (n + 1) * per_cut):
            summed[f] = summed[f] + last[f]
        part = pl.ds(n * per_cut, per_cut)
        copy = pltpu.make_async_remote_copy(
            src_ref=summed.at[part, far],
            dst_ref=partner_in.at[part],
            send_sem=pair_send,
            recv_sem=pair_recv.at[n],
            device_id=(other, dom),
            device_id_type=MESH,
        )
        copy.start()
        pair_copies.append(copy)

    surface_num = jnp.sum(totals[0], axis=1, keepdims=True)
    surface_den = jnp.sum(totals[1])
    small[4].wait()
    small[5].wait()
    air_row = air[...].reshape(1, air_cells)
    inverse = 1.0 / air_row
    ocean_part = fraction[pl.ds(2, 1), :] * ocean[...]
    wet = air_row * ocean_part
    wet = sum(wet[:, q * 128 : (q + 1) * 128] for q in range(lane_tiles))
    air_den = jnp.sum(air_row)
    spot = lax.broadcasted_iota(jnp.int32, (fields, 128), 1)
    line = lax.broadcasted_iota(jnp.int32, (fields, 128), 0)
    stat = jnp.where(spot == line + 16 * comp, surface_num, 0.0)
    stat = jnp.sum(stat, axis=0, keepdims=True)
    spot1 = lax.broadcasted_iota(jnp.int32, (1, 128), 1)
    lead = spot1 - 64
    stat = stat + jnp.where((lead >= 16 * comp) & (lead < 16 * comp + 16), surface_den, 0.0)
    stat = stat + jnp.where(
        (lead >= 16 * groups) & (lead < 16 * groups + 16), air_den, 0.0
    )

    pltpu.make_async_remote_copy(
        src_ref=rows_in.at[pl.ds(0, (domains - 1) * groups * lane_tiles)],
        dst_ref=rows_in.at[pl.ds(0, (domains - 1) * groups * lane_tiles)],
        send_sem=row_send,
        recv_sem=row_recv,
        device_id=(other, dom),
        device_id_type=MESH,
    ).wait_recv()

    def shares(c):
        return [
            rows_in[pl.ds(c * lane_tiles + q, domains, stride=8), :]
            for q in range(lane_tiles)
        ]

    share_own = shares(comp)
    share_other = shares(other)

    half = domains // 2
    side = dom // half
    seat = dom % half
    bit = 1 + comp
    flip = dom // bit % 2
    neighbour = dom + bit * (1 - 2 * flip)

    def across(m, value):
        one = 2 * m + value
        two = m // 2 * 4 + 2 * value + m % 2
        return (1 - side) * half + one + comp * (two - one)

    rank = seat // 2 + comp * (seat // 4 * 2 + seat % 2 - seat // 2)
    mates_here = [side * half + k + jnp.where(seat <= k, 1, 0) for k in range(half - 1)]

    def message(src, dst, p, sem):
        return pltpu.make_async_remote_copy(
            src_ref=src.at[pl.ds(0, body_rows + 1)],
            dst_ref=dst.at[pl.ds(0, body_rows + 1)],
            send_sem=main_send,
            recv_sem=main_recv.at[sem],
            device_id=(comp, p),
            device_id_type=MESH,
        )

    def relay_copy(m):
        return message(
            outgoing.at[across(m, 1 - flip)], relayed.at[m], neighbour, 3 + m
        )

    def direct_copy(p, kind, slot):
        return message(outgoing.at[p], incoming.at[slot], p, kind)

    def wait_all(kind, count):
        block = incoming.at[pl.ds(0, count), pl.ds(0, body_rows + 1)]
        pltpu.make_async_remote_copy(
            src_ref=block,
            dst_ref=block,
            send_sem=main_send,
            recv_sem=main_recv.at[kind],
            device_id=(other, dom),
            device_id_type=MESH,
        ).wait_recv()

    def stat_copy(p, slot):
        return pltpu.make_async_remote_copy(
            src_ref=stat_out,
            dst_ref=stat_in.at[slot],
            send_sem=stat_send,
            recv_sem=stat_recv,
            device_id=(other, p),
            device_id_type=MESH,
        )

    for n in range(PAIR_CUTS):
        pair_copies[n].wait_recv()
        for f in range(n * per_cut, (n + 1) * per_cut):
            acc = None
            for q in range(lane_tiles):
                cut = pl.ds(q * 128, 128)
                both = share_own[q] * summed[f, own, cut]
                both = both + share_other[q] * partner_in[f, :, cut]
                outgoing[:, q * fields + f, :] = both
                acc = both if acc is None else acc + both
            air_parts[pl.ds(f, 1), :] = jnp.sum(acc, axis=0, keepdims=True)
    air_num = jnp.sum(air_parts[...] + wet, axis=1, keepdims=True)
    air_num = jnp.where(spot == line + 16 * groups, air_num, 0.0)
    stat = stat + jnp.sum(air_num, axis=0, keepdims=True)
    outgoing[:, body_rows, :] = jnp.broadcast_to(stat, (domains, 128))
    stat_out[...] = stat
    def at_once(target):
        return (dom >= 2 * quarter) & (target == 0)

    def send_side():
        for p in mates_here[1:]:
            direct_copy(p, 0, seat).start()

    for m in range(half // 2):
        target = across(m, 1 - flip)

        @pl.when(at_once(target))
        def _(target=target):
            direct_copy(target, 2, domains - half // 2 + rank).start()

        @pl.when(jnp.logical_not(at_once(target)))
        def _(m=m):
            relay_copy(m).start()

    direct_copy(mates_here[0], 0, seat).start()
    for k in range(domains):
        stat_copy(k, dom).start()
    for m in range(half // 2):
        for at, where in zip(SIDE_AT, range(2)):
            if m == at:
                pl.when(side == where)(send_side)
        target = across(m, flip)

        @pl.when(jnp.logical_not(at_once(target)))
        def _(m=m, target=target):
            relay_copy(m).wait_recv()
            outgoing[target] = outgoing[target] + relayed[m]

        direct_copy(target, 1, half + rank).start()
    pl.when(side == 1)(send_side)

    def gathered(slots_in):
        body = [
            sum(incoming[slot, pl.ds(q * fields, fields), :] for slot in slots_in)
            for q in range(lane_tiles)
        ]
        return body, sum(incoming[slot, pl.ds(body_rows, 1), :] for slot in slots_in)

    wait_all(0, half - 1)
    sums, stat = gathered([p % half for p in mates_here])

    @pl.when(dom == 0)
    def _():
        wait_all(2, half // 2)
        for m in range(half // 2):
            outgoing[dom] = outgoing[dom] + incoming[domains - half // 2 + m]

    sums = [s + outgoing[dom, pl.ds(q * fields, fields), :] for q, s in enumerate(sums)]
    stat = stat + outgoing[dom, pl.ds(body_rows, 1), :]
    wait_all(1, half // 2)
    late, late_stat = gathered(range(half, half + half // 2))
    sums = [a + b for a, b in zip(sums, late)]
    stat = stat + late_stat
    for q in range(lane_tiles):
        cut = slice(q * 128, (q + 1) * 128)
        merged_ref[:, cut] = sums[q] * inverse[:, cut] + ocean_part[:, cut]

    pltpu.make_async_remote_copy(
        src_ref=stat_in,
        dst_ref=stat_in,
        send_sem=stat_send,
        recv_sem=stat_recv,
        device_id=(other, dom),
        device_id_type=MESH,
    ).wait_recv()
    stat = stat + jnp.sum(stat_in[...], axis=0)
    mean = stat / pltpu.roll(stat, 64, 1)
    for c in range(groups + 1):
        moved = mean if c == 0 else pltpu.roll(mean, 128 - 16 * c, 1)
        means_ref[pl.ds(c, 1), :] = moved[:, :fields]

    pltpu.make_async_remote_copy(
        src_ref=rows_in.at[pl.ds(0, (domains - 1) * groups * lane_tiles)],
        dst_ref=rows_in.at[pl.ds(0, (domains - 1) * groups * lane_tiles)],
        send_sem=row_send,
        recv_sem=row_recv,
        device_id=(other, dom),
        device_id_type=MESH,
    ).wait_send()
    pltpu.make_async_remote_copy(
        src_ref=partner_in,
        dst_ref=partner_in,
        send_sem=pair_send,
        recv_sem=pair_recv.at[0],
        device_id=(other, dom),
        device_id_type=MESH,
    ).wait_send()
    pltpu.make_async_remote_copy(
        src_ref=stat_in,
        dst_ref=stat_in,
        send_sem=stat_send,
        recv_sem=stat_recv,
        device_id=(other, dom),
        device_id_type=MESH,
    ).wait_send()
    pltpu.make_async_remote_copy(
        src_ref=outgoing.at[pl.ds(0, domains - 1), pl.ds(0, body_rows + 1)],
        dst_ref=outgoing.at[pl.ds(0, domains - 1), pl.ds(0, body_rows + 1)],
        send_sem=main_send,
        recv_sem=main_recv.at[0],
        device_id=(other, dom),
        device_id_type=MESH,
    ).wait_send()


def finish(merged_in, means_in, merged_hbm, means_hbm, sem):
    copies = [
        pltpu.make_async_copy(merged_in, merged_hbm, sem.at[0]),
        pltpu.make_async_copy(means_in, means_hbm, sem.at[1]),
    ]
    for copy in copies:
        copy.start()
    for copy in copies:
        copy.wait()


def on_device(
    surface_flux,
    active_mask,
    source_area,
    tile_targets,
    remap_tiles,
    ocean_flux,
    air_fraction,
    air_area,
):
    groups = lax.axis_size("comp")
    domains = lax.axis_size("dom")
    owners = groups * domains
    fields = surface_flux.shape[1]
    cells = surface_flux.shape[2]
    blocks, slots, block_cells, air_cells = remap_tiles.shape
    lane_tiles = air_cells // 128
    message = -(-(lane_tiles * fields + 1) // 8) * 8
    vmem = pl.BlockSpec(memory_space=pltpu.VMEM)
    hbm = pl.BlockSpec(memory_space=pltpu.HBM)
    dma = pltpu.SemaphoreType.DMA
    parts = pl.pallas_call(
        functools.partial(kernel, groups, domains),
        out_shape=(
            pltpu.VMEM((fields, air_cells), F32),
            pltpu.VMEM((groups + 1, fields), F32),
        ),
        in_specs=[hbm] * 8,
        out_specs=(vmem, vmem),
        scratch_shapes=[
            pltpu.VMEM(surface_flux.shape, F32),
            pltpu.VMEM((1, cells), jnp.int32),
            pltpu.VMEM((1, cells), F32),
            pltpu.VMEM((slots, blocks), jnp.int32),
            pltpu.VMEM(remap_tiles.shape, F32),
            pltpu.VMEM(ocean_flux.shape, F32),
            pltpu.VMEM(air_fraction.shape, F32),
            pltpu.VMEM((air_cells,), F32),
            pltpu.VMEM((2 * fields, cells), F32),
            pltpu.VMEM((4 * fields, 2 * cells), BF16),
            pltpu.VMEM((lane_tiles, blocks * slots * fields, 128), F32),
            pltpu.VMEM((1, blocks * slots), jnp.int32),
            pltpu.VMEM((groups * lane_tiles, 128), F32),
            pltpu.VMEM((domains * 8, 128), F32),
            pltpu.VMEM((fields, owners, air_cells), F32),
            pltpu.VMEM((fields, 128), F32),
            pltpu.VMEM((fields, domains, air_cells), F32),
            pltpu.VMEM((1, 128), F32),
            pltpu.VMEM((domains, 1, 128), F32),
            pltpu.VMEM((domains, message, 128), F32),
            pltpu.VMEM((domains, message, 128), F32),
            pltpu.VMEM((domains // 4, message, 128), F32),
            dma((PARTS,)),
            dma((sum(len(c) for c in plan(blocks)[0]),)),
            dma((5,)),
            dma,
            dma,
            dma,
            dma((PAIR_CUTS,)),
            dma,
            dma,
            dma,
            dma((3 + domains // 4,)),
        ],
        compiler_params=pltpu.CompilerParams(
            collective_id=0, has_side_effects=True, vmem_limit_bytes=60 * 1024 * 1024
        ),
    )(
        surface_flux,
        active_mask.reshape(1, cells),
        source_area.reshape(1, cells),
        tile_targets.T,
        remap_tiles,
        ocean_flux,
        air_fraction,
        air_area,
    )
    return pl.pallas_call(
        finish,
        out_shape=(
            jax.ShapeDtypeStruct((fields, air_cells), F32),
            jax.ShapeDtypeStruct((groups + 1, fields), F32),
        ),
        in_specs=[vmem, vmem],
        out_specs=(hbm, hbm),
        scratch_shapes=[dma((2,))],
    )(*[pltpu.with_memory_space_constraint(p, pltpu.VMEM) for p in parts])


def solution(mesh):
    in_specs = (
        P(None, None, ("comp", "dom")),
        P(("comp", "dom")),
        P(("comp", "dom")),
        P(("comp", "dom"), None),
        P(("comp", "dom"), None, None, None),
        P(None, ("comp", "dom")),
        P(None, ("comp", "dom")),
        P(("comp", "dom")),
    )
    out_specs = (P(None, ("comp", "dom")), P())
    return jax.shard_map(
        on_device, mesh=mesh, in_specs=in_specs, out_specs=out_specs, check_vma=False
    )
```

```python
import functools

import jax
import jax.numpy as jnp
from jax import lax
from jax.experimental import pallas as pl
from jax.experimental.pallas import tpu as pltpu
from jax.sharding import PartitionSpec as P

MESH = pl.DeviceIdType.MESH
F32 = jnp.float32
BF16 = jnp.bfloat16
DEPTH = 5
TURNS = (1, 2, 3)
PARTS = 4
UNROLL = 8
PAIR_CUTS = 3
SIDE_AT = (0, 99)


def split(x):
    hi = x.astype(BF16)
    lo = (x - hi.astype(F32)).astype(BF16)
    return hi, lo


def plan(blocks):
    whole = blocks // PARTS
    rounds = [[whole // 2] * 2] + [[whole]] * (PARTS - 2) + [[whole // 2, whole // 4, whole // 4]]
    return rounds, rounds


def kernel(
    groups,
    domains,
    flux_hbm,
    mask_hbm,
    area_hbm,
    targets_hbm,
    tiles_hbm,
    ocean_hbm,
    fraction_hbm,
    air_hbm,
    merged_ref,
    means_ref,
    flux,
    mask,
    area,
    targets,
    tiles,
    ocean,
    fraction,
    air,
    stacked,
    lhs,
    contrib,
    picks,
    row_out,
    rows_in,
    summed,
    air_parts,
    partner_in,
    stat_out,
    stat_in,
    outgoing,
    incoming,
    relayed,
    flux_sem,
    tile_sem,
    small_sem,
    row_send,
    row_recv,
    pair_send,
    pair_recv,
    stat_send,
    stat_recv,
    main_send,
    main_recv,
):
    steps, fields, cells = flux.shape
    blocks, slots, block_cells, air_cells = tiles.shape
    owners = groups * domains
    copy_plan, round_plan = plan(blocks)
    lane_tiles = air_cells // 128
    body_rows = lane_tiles * fields
    comp = lax.axis_index("comp")
    dom = lax.axis_index("dom")
    other = 1 - comp

    small = [
        pltpu.make_async_copy(src, dst, small_sem.at[i])
        for i, src, dst in (
            [
                (0, fraction_hbm, fraction),
                (1, mask_hbm, mask),
                (1, area_hbm, area),
                (2, targets_hbm, targets),
                (3, ocean_hbm, ocean),
                (4, air_hbm, air),
            ]
        )
    ]
    for copy in small[1:3]:
        copy.start()
    flux_width = cells // PARTS
    flux_copies = []
    tile_copies = []
    waiting = []
    low = 0
    for i in range(PARTS):
        part = pl.ds(i * flux_width, flux_width)
        flux_copies.append(
            pltpu.make_async_copy(flux_hbm.at[:, :, part], flux.at[:, :, part], flux_sem.at[i])
        )
        for size in copy_plan[i]:
            part = pl.ds(low, size)
            low += size
            copy = pltpu.make_async_copy(
                tiles_hbm.at[part], tiles.at[part], tile_sem.at[len(tile_copies)]
            )
            tile_copies.append((low, copy))
            waiting.append(copy)

    def start_more(count):
        for copy in waiting[:count]:
            copy.start(priority=1)
        del waiting[:count]

    for copy in flux_copies:
        copy.start()
    start_more(DEPTH)
    small[0].start()

    barrier = pltpu.get_barrier_semaphore()
    rivals = []
    for k in range(domains - 1):
        rivals.append((comp, k + jnp.where(dom <= k, 1, 0)))
    mates = [(other, k) for k in range(domains)]
    for a, b in zip(rivals + [None], mates):
        for peer in (a, b):
            if peer is not None:
                pl.semaphore_signal(barrier, inc=1, device_id=peer, device_id_type=MESH)

    both_rows = contrib.at[0, pl.ds(0, 2 * cells // 128)]
    pltpu.make_async_copy(both_rows, both_rows, small_sem.at[1]).wait()
    width = min(512, flux_width)
    lane = lax.broadcasted_iota(jnp.int32, (fields, width), 1)
    first = lax.rem(lane, 2 * block_cells) < block_cells

    def weigh(i, carry):
        total, area_total = carry
        part = pl.ds(pl.multiple_of(i * width, width), width)
        value = flux[0, :, part]
        for s in range(1, steps):
            value = value + flux[s, :, part]
        a = area[:, part]
        value = (value / steps) * (mask[:, part].astype(F32) * a)
        stacked[pl.ds(0, fields), part] = jnp.where(first, value, 0.0)
        stacked[pl.ds(fields, fields), part] = jnp.where(first, 0.0, value)
        both = stacked[:, part]
        hi = both.astype(BF16).astype(F32)
        left = jnp.concatenate([hi, both - hi], axis=0).astype(BF16)
        right = jnp.concatenate([hi, jnp.zeros_like(hi)], axis=0).astype(BF16)
        for j in range(width // 128):
            cut = slice(j * 128, (j + 1) * 128)
            base = pl.multiple_of(2 * i * width + 256 * j, 256)
            lhs[:, pl.ds(base, 128)] = left[:, cut]
            lhs[:, pl.ds(base + 128, 128)] = right[:, cut]
        return total + value, area_total + a

    early = blocks - blocks // PARTS

    def pair(j, carry):
        left = lhs[:, pl.ds(pl.multiple_of(j * 256, 256), 256)]
        right = []
        for t in range(slots):
            weights = tiles[pl.ds(2 * j, 2), t].reshape(2 * block_cells, air_cells)
            hi, lo = split(weights)
            right.append(jnp.concatenate([hi, lo], axis=0))
        r = jnp.dot(left, jnp.concatenate(right, axis=1), preferred_element_type=F32)
        r = r[: 2 * fields] + r[2 * fields :]
        for t in range(slots):
            base = pl.multiple_of((t * carry[1] + carry[0] + 2 * j) * fields, 2 * fields)
            for q in range(lane_tiles):
                n = t * lane_tiles + q
                contrib[q, pl.ds(base, 2 * fields), :] = r[:, n * 128 : (n + 1) * 128]
        return carry

    def select(low, count):
        for t in range(slots):
            picks[:, pl.ds(2 * low + t * count, count)] = targets[pl.ds(t, 1), pl.ds(low, count)]
        tile_ids = picks[:, pl.ds(2 * low, slots * count)]
        owner_ids = lax.broadcasted_iota(jnp.int32, (owners, slots * count), 0)
        return jnp.where(owner_ids == tile_ids, 1.0, 0.0).astype(BF16)

    def collect(low, count, selector, g):
        right = []
        for f in (2 * g, 2 * g + 1):
            for q in range(lane_tiles):
                rows = pl.ds(slots * low * fields + f, slots * count, stride=fields)
                right.append(split(contrib[q, rows, :]))
        his = jnp.concatenate([r[0] for r in right], axis=1)
        los = jnp.concatenate([r[1] for r in right], axis=1)
        s = jnp.dot(selector, his, preferred_element_type=F32)
        s = s + jnp.dot(selector, los, preferred_element_type=F32)
        return [s[:, n * air_cells : (n + 1) * air_cells] for n in range(2)]

    def row_copy(p, slot):
        return pltpu.make_async_remote_copy(
            src_ref=row_out,
            dst_ref=rows_in.at[pl.ds(pl.multiple_of(slot * 8, 8), groups * lane_tiles)],
            send_sem=row_send,
            recv_sem=row_recv,
            device_id=(comp, p),
            device_id_type=MESH,
        )

    def send_rows():
        small[0].wait()
        for c in range(groups):
            for q in range(lane_tiles):
                row = fraction[pl.ds(c, 1), pl.ds(q * 128, 128)]
                row_out[pl.ds(c * lane_tiles + q, 1), :] = row
                rows_in[pl.ds(dom * 8 + c * lane_tiles + q, 1), :] = row
        pl.semaphore_wait(barrier, owners - 1)
        for c, p in rivals:
            row_copy(p, dom).start()

    quarter = domains // 4
    turns = [
        (TURNS[0], (3 * quarter, domains)),
        (TURNS[1], (2 * quarter, 3 * quarter)),
        (TURNS[2], (1, 2 * quarter)),
    ]

    totals = (jnp.zeros((fields, width), F32), jnp.zeros((1, width), F32))
    weigh_rounds = flux_width // width
    low = 0
    arrived = 0
    step = 0
    for i in range(PARTS):
        flux_copies[i].wait()
        if i == 1:
            for copy in small[3:]:
                copy.start()
        totals = lax.fori_loop(
            i * weigh_rounds, (i + 1) * weigh_rounds, weigh, totals, unroll=weigh_rounds
        )
        for size in round_plan[i]:
            for low_dom, high_dom in [span for at, span in turns if at == step]:
                pl.when((dom >= low_dom) & (dom < high_dom))(send_rows)
            step += 1
            while arrived < len(tile_copies) and tile_copies[arrived][0] <= low + size:
                tile_copies[arrived][1].wait()
                start_more(1)
                arrived += 1
            first_block, count = (0, early) if low < early else (early, blocks - early)
            place = (slots * first_block - first_block, count)
            pairs = size // 2
            lax.fori_loop(
                low // 2,
                low // 2 + pairs,
                lambda j, c, place=place: (pair(j, place), c)[1],
                0,
                unroll=min(UNROLL, pairs),
            )
            low += size
        if low == early:
            small[3].wait()
            selector = select(0, early)
            last_selector = select(early, blocks - early)
            for g in range(fields // 2):
                summed[2 * g], summed[2 * g + 1] = collect(0, early, selector, g)

    pl.when(dom == 0)(send_rows)

    far = pl.ds(pl.multiple_of(other * domains, 8), domains)
    own = pl.ds(pl.multiple_of(comp * domains, 8), domains)
    per_cut = fields // PAIR_CUTS
    pair_copies = []
    last = []
    for g in range(fields // 2):
        last.extend(collect(early, blocks - early, last_selector, g))
    for n in range(PAIR_CUTS):
        for f in range(n * per_cut, (n + 1) * per_cut):
            summed[f] = summed[f] + last[f]
        part = pl.ds(n * per_cut, per_cut)
        copy = pltpu.make_async_remote_copy(
            src_ref=summed.at[part, far],
            dst_ref=partner_in.at[part],
            send_sem=pair_send,
            recv_sem=pair_recv.at[n],
            device_id=(other, dom),
            device_id_type=MESH,
        )
        copy.start()
        pair_copies.append(copy)

    surface_num = jnp.sum(totals[0], axis=1, keepdims=True)
    surface_den = jnp.sum(totals[1])
    small[4].wait()
    small[5].wait()
    air_row = air[...].reshape(1, air_cells)
    inverse = 1.0 / air_row
    ocean_part = fraction[pl.ds(2, 1), :] * ocean[...]
    wet = air_row * ocean_part
    wet = sum(wet[:, q * 128 : (q + 1) * 128] for q in range(lane_tiles))
    air_den = jnp.sum(air_row)
    spot = lax.broadcasted_iota(jnp.int32, (fields, 128), 1)
    line = lax.broadcasted_iota(jnp.int32, (fields, 128), 0)
    stat = jnp.where(spot == line + 16 * comp, surface_num, 0.0)
    stat = jnp.sum(stat, axis=0, keepdims=True)
    spot1 = lax.broadcasted_iota(jnp.int32, (1, 128), 1)
    lead = spot1 - 64
    stat = stat + jnp.where((lead >= 16 * comp) & (lead < 16 * comp + 16), surface_den, 0.0)
    stat = stat + jnp.where(
        (lead >= 16 * groups) & (lead < 16 * groups + 16), air_den, 0.0
    )

    pltpu.make_async_remote_copy(
        src_ref=rows_in.at[pl.ds(0, (domains - 1) * groups * lane_tiles)],
        dst_ref=rows_in.at[pl.ds(0, (domains - 1) * groups * lane_tiles)],
        send_sem=row_send,
        recv_sem=row_recv,
        device_id=(other, dom),
        device_id_type=MESH,
    ).wait_recv()

    def shares(c):
        return [
            rows_in[pl.ds(c * lane_tiles + q, domains, stride=8), :]
            for q in range(lane_tiles)
        ]

    share_own = shares(comp)
    share_other = shares(other)

    half = domains // 2
    side = dom // half
    seat = dom % half
    bit = 1 + comp
    flip = dom // bit % 2
    neighbour = dom + bit * (1 - 2 * flip)

    def across(m, value):
        one = 2 * m + value
        two = m // 2 * 4 + 2 * value + m % 2
        return (1 - side) * half + one + comp * (two - one)

    rank = seat // 2 + comp * (seat // 4 * 2 + seat % 2 - seat // 2)
    mates_here = [side * half + k + jnp.where(seat <= k, 1, 0) for k in range(half - 1)]

    def message(src, dst, p, sem):
        return pltpu.make_async_remote_copy(
            src_ref=src.at[pl.ds(0, body_rows + 1)],
            dst_ref=dst.at[pl.ds(0, body_rows + 1)],
            send_sem=main_send,
            recv_sem=main_recv.at[sem],
            device_id=(comp, p),
            device_id_type=MESH,
        )

    def relay_copy(m):
        return message(
            outgoing.at[across(m, 1 - flip)], relayed.at[m], neighbour, 3 + m
        )

    def direct_copy(p, kind, slot):
        return message(outgoing.at[p], incoming.at[slot], p, kind)

    def wait_all(kind, count):
        block = incoming.at[pl.ds(0, count), pl.ds(0, body_rows + 1)]
        pltpu.make_async_remote_copy(
            src_ref=block,
            dst_ref=block,
            send_sem=main_send,
            recv_sem=main_recv.at[kind],
            device_id=(other, dom),
            device_id_type=MESH,
        ).wait_recv()

    def stat_copy(p, slot):
        return pltpu.make_async_remote_copy(
            src_ref=stat_out,
            dst_ref=stat_in.at[slot],
            send_sem=stat_send,
            recv_sem=stat_recv,
            device_id=(other, p),
            device_id_type=MESH,
        )

    for n in range(PAIR_CUTS):
        pair_copies[n].wait_recv()
        for f in range(n * per_cut, (n + 1) * per_cut):
            acc = None
            for q in range(lane_tiles):
                cut = pl.ds(q * 128, 128)
                both = share_own[q] * summed[f, own, cut]
                both = both + share_other[q] * partner_in[f, :, cut]
                outgoing[:, q * fields + f, :] = both
                acc = both if acc is None else acc + both
            air_parts[pl.ds(f, 1), :] = jnp.sum(acc, axis=0, keepdims=True)
    air_num = jnp.sum(air_parts[...] + wet, axis=1, keepdims=True)
    air_num = jnp.where(spot == line + 16 * groups, air_num, 0.0)
    stat = stat + jnp.sum(air_num, axis=0, keepdims=True)
    outgoing[:, body_rows, :] = jnp.broadcast_to(stat, (domains, 128))
    stat_out[...] = stat
    def at_once(target):
        return (dom >= 2 * quarter) & (target == 0)

    def send_side():
        for p in mates_here[1:]:
            direct_copy(p, 0, seat).start()

    for m in range(half // 2):
        target = across(m, 1 - flip)

        @pl.when(at_once(target))
        def _(target=target):
            direct_copy(target, 2, domains - half // 2 + rank).start()

        @pl.when(jnp.logical_not(at_once(target)))
        def _(m=m):
            relay_copy(m).start()

    direct_copy(mates_here[0], 0, seat).start()
    for k in range(domains):
        stat_copy(k, dom).start()
    for m in range(half // 2):
        for at, where in zip(SIDE_AT, range(2)):
            if m == at:
                pl.when(side == where)(send_side)
        target = across(m, flip)

        @pl.when(jnp.logical_not(at_once(target)))
        def _(m=m, target=target):
            relay_copy(m).wait_recv()
            outgoing[target] = outgoing[target] + relayed[m]

        direct_copy(target, 1, half + rank).start()
    pl.when(side == 1)(send_side)

    def gathered(slots_in):
        body = [
            sum(incoming[slot, pl.ds(q * fields, fields), :] for slot in slots_in)
            for q in range(lane_tiles)
        ]
        return body, sum(incoming[slot, pl.ds(body_rows, 1), :] for slot in slots_in)

    wait_all(0, half - 1)
    sums, stat = gathered([p % half for p in mates_here])

    @pl.when(dom == 0)
    def _():
        wait_all(2, half // 2)
        for m in range(half // 2):
            outgoing[dom] = outgoing[dom] + incoming[domains - half // 2 + m]

    sums = [s + outgoing[dom, pl.ds(q * fields, fields), :] for q, s in enumerate(sums)]
    stat = stat + outgoing[dom, pl.ds(body_rows, 1), :]
    pltpu.make_async_remote_copy(
        src_ref=stat_in,
        dst_ref=stat_in,
        send_sem=stat_send,
        recv_sem=stat_recv,
        device_id=(other, dom),
        device_id_type=MESH,
    ).wait_recv()
    stat = stat + jnp.sum(stat_in[...], axis=0)
    wait_all(1, half // 2)
    late, late_stat = gathered(range(half, half + half // 2))
    sums = [a + b for a, b in zip(sums, late)]
    stat = stat + late_stat
    for q in range(lane_tiles):
        cut = slice(q * 128, (q + 1) * 128)
        merged_ref[:, cut] = sums[q] * inverse[:, cut] + ocean_part[:, cut]

    mean = stat / pltpu.roll(stat, 64, 1)
    for c in range(groups + 1):
        moved = mean if c == 0 else pltpu.roll(mean, 128 - 16 * c, 1)
        means_ref[pl.ds(c, 1), :] = moved[:, :fields]

    pltpu.make_async_remote_copy(
        src_ref=rows_in.at[pl.ds(0, (domains - 1) * groups * lane_tiles)],
        dst_ref=rows_in.at[pl.ds(0, (domains - 1) * groups * lane_tiles)],
        send_sem=row_send,
        recv_sem=row_recv,
        device_id=(other, dom),
        device_id_type=MESH,
    ).wait_send()
    pltpu.make_async_remote_copy(
        src_ref=partner_in,
        dst_ref=partner_in,
        send_sem=pair_send,
        recv_sem=pair_recv.at[0],
        device_id=(other, dom),
        device_id_type=MESH,
    ).wait_send()
    pltpu.make_async_remote_copy(
        src_ref=stat_in,
        dst_ref=stat_in,
        send_sem=stat_send,
        recv_sem=stat_recv,
        device_id=(other, dom),
        device_id_type=MESH,
    ).wait_send()
    pltpu.make_async_remote_copy(
        src_ref=outgoing.at[pl.ds(0, domains - 1), pl.ds(0, body_rows + 1)],
        dst_ref=outgoing.at[pl.ds(0, domains - 1), pl.ds(0, body_rows + 1)],
        send_sem=main_send,
        recv_sem=main_recv.at[0],
        device_id=(other, dom),
        device_id_type=MESH,
    ).wait_send()


def finish(merged_in, means_in, merged_hbm, means_hbm, sem):
    copies = [
        pltpu.make_async_copy(merged_in, merged_hbm, sem.at[0]),
        pltpu.make_async_copy(means_in, means_hbm, sem.at[1]),
    ]
    for copy in copies:
        copy.start()
    for copy in copies:
        copy.wait()


def on_device(
    surface_flux,
    active_mask,
    source_area,
    tile_targets,
    remap_tiles,
    ocean_flux,
    air_fraction,
    air_area,
):
    groups = lax.axis_size("comp")
    domains = lax.axis_size("dom")
    owners = groups * domains
    fields = surface_flux.shape[1]
    cells = surface_flux.shape[2]
    blocks, slots, block_cells, air_cells = remap_tiles.shape
    lane_tiles = air_cells // 128
    message = -(-(lane_tiles * fields + 1) // 8) * 8
    vmem = pl.BlockSpec(memory_space=pltpu.VMEM)
    hbm = pl.BlockSpec(memory_space=pltpu.HBM)
    dma = pltpu.SemaphoreType.DMA
    parts = pl.pallas_call(
        functools.partial(kernel, groups, domains),
        out_shape=(
            pltpu.VMEM((fields, air_cells), F32),
            pltpu.VMEM((groups + 1, fields), F32),
        ),
        in_specs=[hbm] * 8,
        out_specs=(vmem, vmem),
        scratch_shapes=[
            pltpu.VMEM(surface_flux.shape, F32),
            pltpu.VMEM((1, cells), jnp.int32),
            pltpu.VMEM((1, cells), F32),
            pltpu.VMEM((slots, blocks), jnp.int32),
            pltpu.VMEM(remap_tiles.shape, F32),
            pltpu.VMEM(ocean_flux.shape, F32),
            pltpu.VMEM(air_fraction.shape, F32),
            pltpu.VMEM((air_cells,), F32),
            pltpu.VMEM((2 * fields, cells), F32),
            pltpu.VMEM((4 * fields, 2 * cells), BF16),
            pltpu.VMEM((lane_tiles, blocks * slots * fields, 128), F32),
            pltpu.VMEM((1, blocks * slots), jnp.int32),
            pltpu.VMEM((groups * lane_tiles, 128), F32),
            pltpu.VMEM((domains * 8, 128), F32),
            pltpu.VMEM((fields, owners, air_cells), F32),
            pltpu.VMEM((fields, 128), F32),
            pltpu.VMEM((fields, domains, air_cells), F32),
            pltpu.VMEM((1, 128), F32),
            pltpu.VMEM((domains, 1, 128), F32),
            pltpu.VMEM((domains, message, 128), F32),
            pltpu.VMEM((domains, message, 128), F32),
            pltpu.VMEM((domains // 4, message, 128), F32),
            dma((PARTS,)),
            dma((sum(len(c) for c in plan(blocks)[0]),)),
            dma((5,)),
            dma,
            dma,
            dma,
            dma((PAIR_CUTS,)),
            dma,
            dma,
            dma,
            dma((3 + domains // 4,)),
        ],
        compiler_params=pltpu.CompilerParams(
            collective_id=0, has_side_effects=True, vmem_limit_bytes=60 * 1024 * 1024
        ),
    )(
        surface_flux,
        active_mask.reshape(1, cells),
        source_area.reshape(1, cells),
        tile_targets.T,
        remap_tiles,
        ocean_flux,
        air_fraction,
        air_area,
    )
    return pl.pallas_call(
        finish,
        out_shape=(
            jax.ShapeDtypeStruct((fields, air_cells), F32),
            jax.ShapeDtypeStruct((groups + 1, fields), F32),
        ),
        in_specs=[vmem, vmem],
        out_specs=(hbm, hbm),
        scratch_shapes=[dma((2,))],
    )(*[pltpu.with_memory_space_constraint(p, pltpu.VMEM) for p in parts])


def solution(mesh):
    in_specs = (
        P(None, None, ("comp", "dom")),
        P(("comp", "dom")),
        P(("comp", "dom")),
        P(("comp", "dom"), None),
        P(("comp", "dom"), None, None, None),
        P(None, ("comp", "dom")),
        P(None, ("comp", "dom")),
        P(("comp", "dom")),
    )
    out_specs = (P(None, ("comp", "dom")), P())
    return jax.shard_map(
        on_device, mesh=mesh, in_specs=in_specs, out_specs=out_specs, check_vma=False
    )
```

```python
import functools

import jax
import jax.numpy as jnp
from jax import lax
from jax.experimental import pallas as pl
from jax.experimental.pallas import tpu as pltpu
from jax.sharding import PartitionSpec as P

MESH = pl.DeviceIdType.MESH
F32 = jnp.float32
BF16 = jnp.bfloat16
DEPTH = 5
TURNS = (1, 2, 3)
PARTS = 4
UNROLL = 8
PAIR_CUTS = 3
SIDE_AT = (0, 99)


def split(x):
    hi = x.astype(BF16)
    lo = (x - hi.astype(F32)).astype(BF16)
    return hi, lo


def plan(blocks):
    whole = blocks // PARTS
    rounds = [[whole // 2] * 2] + [[whole]] * (PARTS - 2) + [[whole // 2, whole // 2]]
    return rounds, rounds


def kernel(
    groups,
    domains,
    flux_hbm,
    mask_hbm,
    area_hbm,
    targets_hbm,
    tiles_hbm,
    ocean_hbm,
    fraction_hbm,
    air_hbm,
    merged_ref,
    means_ref,
    flux,
    mask,
    area,
    targets,
    tiles,
    ocean,
    fraction,
    air,
    stacked,
    lhs,
    contrib,
    picks,
    row_out,
    rows_in,
    summed,
    air_parts,
    partner_in,
    stat_out,
    stat_in,
    outgoing,
    incoming,
    relayed,
    flux_sem,
    tile_sem,
    small_sem,
    row_send,
    row_recv,
    pair_send,
    pair_recv,
    stat_send,
    stat_recv,
    main_send,
    main_recv,
):
    steps, fields, cells = flux.shape
    blocks, slots, block_cells, air_cells = tiles.shape
    owners = groups * domains
    copy_plan, round_plan = plan(blocks)
    lane_tiles = air_cells // 128
    body_rows = lane_tiles * fields
    comp = lax.axis_index("comp")
    dom = lax.axis_index("dom")
    other = 1 - comp

    small = [
        pltpu.make_async_copy(src, dst, small_sem.at[i])
        for i, src, dst in (
            [
                (0, fraction_hbm, fraction),
                (1, mask_hbm, mask),
                (1, area_hbm, area),
                (2, targets_hbm, targets),
                (3, ocean_hbm, ocean),
                (4, air_hbm, air),
            ]
        )
    ]
    for copy in small[1:3]:
        copy.start()
    flux_width = cells // PARTS
    flux_copies = []
    tile_copies = []
    waiting = []
    low = 0
    for i in range(PARTS):
        part = pl.ds(i * flux_width, flux_width)
        flux_copies.append(
            pltpu.make_async_copy(flux_hbm.at[:, :, part], flux.at[:, :, part], flux_sem.at[i])
        )
        for size in copy_plan[i]:
            part = pl.ds(low, size)
            low += size
            copy = pltpu.make_async_copy(
                tiles_hbm.at[part], tiles.at[part], tile_sem.at[len(tile_copies)]
            )
            tile_copies.append((low, copy))
            waiting.append(copy)

    def start_more(count):
        for copy in waiting[:count]:
            copy.start(priority=1)
        del waiting[:count]

    for copy in flux_copies:
        copy.start()
    start_more(DEPTH)
    small[0].start()

    barrier = pltpu.get_barrier_semaphore()
    rivals = []
    for k in range(domains - 1):
        rivals.append((comp, k + jnp.where(dom <= k, 1, 0)))
    mates = [(other, k) for k in range(domains)]
    for a, b in zip(rivals + [None], mates):
        for peer in (a, b):
            if peer is not None:
                pl.semaphore_signal(barrier, inc=1, device_id=peer, device_id_type=MESH)

    both_rows = contrib.at[0, pl.ds(0, 2 * cells // 128)]
    pltpu.make_async_copy(both_rows, both_rows, small_sem.at[1]).wait()
    width = min(512, flux_width)
    lane = lax.broadcasted_iota(jnp.int32, (fields, width), 1)
    first = lax.rem(lane, 2 * block_cells) < block_cells

    def weigh(i, carry):
        total, area_total = carry
        part = pl.ds(pl.multiple_of(i * width, width), width)
        value = flux[0, :, part]
        for s in range(1, steps):
            value = value + flux[s, :, part]
        a = area[:, part]
        value = (value / steps) * (mask[:, part].astype(F32) * a)
        stacked[pl.ds(0, fields), part] = jnp.where(first, value, 0.0)
        stacked[pl.ds(fields, fields), part] = jnp.where(first, 0.0, value)
        both = stacked[:, part]
        hi = both.astype(BF16).astype(F32)
        left = jnp.concatenate([hi, both - hi], axis=0).astype(BF16)
        right = jnp.concatenate([hi, jnp.zeros_like(hi)], axis=0).astype(BF16)
        for j in range(width // 128):
            cut = slice(j * 128, (j + 1) * 128)
            base = pl.multiple_of(2 * i * width + 256 * j, 256)
            lhs[:, pl.ds(base, 128)] = left[:, cut]
            lhs[:, pl.ds(base + 128, 128)] = right[:, cut]
        return total + value, area_total + a

    early = blocks - blocks // PARTS

    def pair(j, carry):
        left = lhs[:, pl.ds(pl.multiple_of(j * 256, 256), 256)]
        right = []
        for t in range(slots):
            weights = tiles[pl.ds(2 * j, 2), t].reshape(2 * block_cells, air_cells)
            hi, lo = split(weights)
            right.append(jnp.concatenate([hi, lo], axis=0))
        r = jnp.dot(left, jnp.concatenate(right, axis=1), preferred_element_type=F32)
        r = r[: 2 * fields] + r[2 * fields :]
        for t in range(slots):
            base = pl.multiple_of((t * carry[1] + carry[0] + 2 * j) * fields, 2 * fields)
            for q in range(lane_tiles):
                n = t * lane_tiles + q
                contrib[q, pl.ds(base, 2 * fields), :] = r[:, n * 128 : (n + 1) * 128]
        return carry

    def select(low, count):
        for t in range(slots):
            picks[:, pl.ds(2 * low + t * count, count)] = targets[pl.ds(t, 1), pl.ds(low, count)]
        tile_ids = picks[:, pl.ds(2 * low, slots * count)]
        owner_ids = lax.broadcasted_iota(jnp.int32, (owners, slots * count), 0)
        return jnp.where(owner_ids == tile_ids, 1.0, 0.0).astype(BF16)

    def collect(low, count, selector, g):
        right = []
        for f in (2 * g, 2 * g + 1):
            for q in range(lane_tiles):
                rows = pl.ds(slots * low * fields + f, slots * count, stride=fields)
                right.append(split(contrib[q, rows, :]))
        his = jnp.concatenate([r[0] for r in right], axis=1)
        los = jnp.concatenate([r[1] for r in right], axis=1)
        s = jnp.dot(selector, his, preferred_element_type=F32)
        s = s + jnp.dot(selector, los, preferred_element_type=F32)
        return [s[:, n * air_cells : (n + 1) * air_cells] for n in range(2)]

    def row_copy(p, slot):
        return pltpu.make_async_remote_copy(
            src_ref=row_out,
            dst_ref=rows_in.at[pl.ds(pl.multiple_of(slot * 8, 8), groups * lane_tiles)],
            send_sem=row_send,
            recv_sem=row_recv,
            device_id=(comp, p),
            device_id_type=MESH,
        )

    def send_rows():
        small[0].wait()
        for c in range(groups):
            for q in range(lane_tiles):
                row = fraction[pl.ds(c, 1), pl.ds(q * 128, 128)]
                row_out[pl.ds(c * lane_tiles + q, 1), :] = row
                rows_in[pl.ds(dom * 8 + c * lane_tiles + q, 1), :] = row
        pl.semaphore_wait(barrier, owners - 1)
        for c, p in rivals:
            row_copy(p, dom).start()

    quarter = domains // 4
    turns = [
        (TURNS[0], (3 * quarter, domains)),
        (TURNS[1], (2 * quarter, 3 * quarter)),
        (TURNS[2], (1, 2 * quarter)),
    ]

    totals = (jnp.zeros((fields, width), F32), jnp.zeros((1, width), F32))
    weigh_rounds = flux_width // width
    low = 0
    arrived = 0
    step = 0
    for i in range(PARTS):
        flux_copies[i].wait()
        if i == 1:
            for copy in small[3:]:
                copy.start()
        totals = lax.fori_loop(
            i * weigh_rounds, (i + 1) * weigh_rounds, weigh, totals, unroll=weigh_rounds
        )
        for size in round_plan[i]:
            for low_dom, high_dom in [span for at, span in turns if at == step]:
                pl.when((dom >= low_dom) & (dom < high_dom))(send_rows)
            step += 1
            while arrived < len(tile_copies) and tile_copies[arrived][0] <= low + size:
                tile_copies[arrived][1].wait()
                start_more(1)
                arrived += 1
            first_block, count = (0, early) if low < early else (early, blocks - early)
            place = (slots * first_block - first_block, count)
            pairs = size // 2
            lax.fori_loop(
                low // 2,
                low // 2 + pairs,
                lambda j, c, place=place: (pair(j, place), c)[1],
                0,
                unroll=min(UNROLL, pairs),
            )
            low += size
        if low == early:
            small[3].wait()
            selector = select(0, early)
            last_selector = select(early, blocks - early)
            for g in range(fields // 2):
                summed[2 * g], summed[2 * g + 1] = collect(0, early, selector, g)

    pl.when(dom == 0)(send_rows)

    far = pl.ds(pl.multiple_of(other * domains, 8), domains)
    own = pl.ds(pl.multiple_of(comp * domains, 8), domains)
    per_cut = fields // PAIR_CUTS
    pair_copies = []
    last = []
    for g in range(fields // 2):
        last.extend(collect(early, blocks - early, last_selector, g))
    for n in range(PAIR_CUTS):
        for f in range(n * per_cut, (n + 1) * per_cut):
            summed[f] = summed[f] + last[f]
        part = pl.ds(n * per_cut, per_cut)
        copy = pltpu.make_async_remote_copy(
            src_ref=summed.at[part, far],
            dst_ref=partner_in.at[part],
            send_sem=pair_send,
            recv_sem=pair_recv.at[n],
            device_id=(other, dom),
            device_id_type=MESH,
        )
        copy.start()
        pair_copies.append(copy)

    surface_num = jnp.sum(totals[0], axis=1, keepdims=True)
    surface_den = jnp.sum(totals[1])
    small[4].wait()
    small[5].wait()
    air_row = air[...].reshape(1, air_cells)
    inverse = 1.0 / air_row
    ocean_part = fraction[pl.ds(2, 1), :] * ocean[...]
    wet = air_row * ocean_part
    wet = sum(wet[:, q * 128 : (q + 1) * 128] for q in range(lane_tiles))
    air_den = jnp.sum(air_row)
    spot = lax.broadcasted_iota(jnp.int32, (fields, 128), 1)
    line = lax.broadcasted_iota(jnp.int32, (fields, 128), 0)
    stat = jnp.where(spot == line + 16 * comp, surface_num, 0.0)
    stat = jnp.sum(stat, axis=0, keepdims=True)
    spot1 = lax.broadcasted_iota(jnp.int32, (1, 128), 1)
    lead = spot1 - 64
    stat = stat + jnp.where((lead >= 16 * comp) & (lead < 16 * comp + 16), surface_den, 0.0)
    stat = stat + jnp.where(
        (lead >= 16 * groups) & (lead < 16 * groups + 16), air_den, 0.0
    )

    pltpu.make_async_remote_copy(
        src_ref=rows_in.at[pl.ds(0, (domains - 1) * groups * lane_tiles)],
        dst_ref=rows_in.at[pl.ds(0, (domains - 1) * groups * lane_tiles)],
        send_sem=row_send,
        recv_sem=row_recv,
        device_id=(other, dom),
        device_id_type=MESH,
    ).wait_recv()

    def shares(c):
        return [
            rows_in[pl.ds(c * lane_tiles + q, domains, stride=8), :]
            for q in range(lane_tiles)
        ]

    share_own = shares(comp)
    share_other = shares(other)

    half = domains // 2
    side = dom // half
    seat = dom % half
    bit = 1 + comp
    flip = dom // bit % 2
    neighbour = dom + bit * (1 - 2 * flip)

    def across(m, value):
        one = 2 * m + value
        two = m // 2 * 4 + 2 * value + m % 2
        return (1 - side) * half + one + comp * (two - one)

    rank = seat // 2 + comp * (seat // 4 * 2 + seat % 2 - seat // 2)
    mates_here = [side * half + k + jnp.where(seat <= k, 1, 0) for k in range(half - 1)]

    def message(src, dst, p, sem):
        return pltpu.make_async_remote_copy(
            src_ref=src.at[pl.ds(0, body_rows + 1)],
            dst_ref=dst.at[pl.ds(0, body_rows + 1)],
            send_sem=main_send,
            recv_sem=main_recv.at[sem],
            device_id=(comp, p),
            device_id_type=MESH,
        )

    def relay_copy(m):
        return message(
            outgoing.at[across(m, 1 - flip)], relayed.at[m], neighbour, 3 + m
        )

    def direct_copy(p, kind, slot):
        return message(outgoing.at[p], incoming.at[slot], p, kind)

    def wait_all(kind, count):
        block = incoming.at[pl.ds(0, count), pl.ds(0, body_rows + 1)]
        pltpu.make_async_remote_copy(
            src_ref=block,
            dst_ref=block,
            send_sem=main_send,
            recv_sem=main_recv.at[kind],
            device_id=(other, dom),
            device_id_type=MESH,
        ).wait_recv()

    def stat_copy(p, slot):
        return pltpu.make_async_remote_copy(
            src_ref=stat_out,
            dst_ref=stat_in.at[slot],
            send_sem=stat_send,
            recv_sem=stat_recv,
            device_id=(other, p),
            device_id_type=MESH,
        )

    for n in range(PAIR_CUTS):
        pair_copies[n].wait_recv()
        for f in range(n * per_cut, (n + 1) * per_cut):
            acc = None
            for q in range(lane_tiles):
                cut = pl.ds(q * 128, 128)
                both = share_own[q] * summed[f, own, cut]
                both = both + share_other[q] * partner_in[f, :, cut]
                outgoing[:, q * fields + f, :] = both
                acc = both if acc is None else acc + both
            air_parts[pl.ds(f, 1), :] = jnp.sum(acc, axis=0, keepdims=True)
    air_num = jnp.sum(air_parts[...] + wet, axis=1, keepdims=True)
    air_num = jnp.where(spot == line + 16 * groups, air_num, 0.0)
    stat = stat + jnp.sum(air_num, axis=0, keepdims=True)
    outgoing[:, body_rows, :] = jnp.broadcast_to(stat, (domains, 128))
    stat_out[...] = stat
    def at_once(target):
        return (dom >= 2 * quarter) & (target == 0)

    def send_side():
        for p in mates_here[1:]:
            direct_copy(p, 0, seat).start()

    for m in range(half // 2):
        target = across(m, 1 - flip)

        @pl.when(at_once(target))
        def _(target=target):
            direct_copy(target, 2, domains - half // 2 + rank).start()

        @pl.when(jnp.logical_not(at_once(target)))
        def _(m=m):
            relay_copy(m).start()

    direct_copy(mates_here[0], 0, seat).start()
    for k in range(domains):
        stat_copy(k, dom).start()
    for m in range(half // 2):
        for at, where in zip(SIDE_AT, range(2)):
            if m == at:
                pl.when(side == where)(send_side)
        target = across(m, flip)

        @pl.when(jnp.logical_not(at_once(target)))
        def _(m=m, target=target):
            relay_copy(m).wait_recv()
            outgoing[target] = outgoing[target] + relayed[m]

        direct_copy(target, 1, half + rank).start()
    pl.when(side == 1)(send_side)

    def gathered(slots_in):
        body = [
            sum(incoming[slot, pl.ds(q * fields, fields), :] for slot in slots_in)
            for q in range(lane_tiles)
        ]
        return body, sum(incoming[slot, pl.ds(body_rows, 1), :] for slot in slots_in)

    wait_all(0, half - 1)
    sums, stat = gathered([p % half for p in mates_here])

    @pl.when(dom == 0)
    def _():
        wait_all(2, half // 2)
        for m in range(half // 2):
            outgoing[dom] = outgoing[dom] + incoming[domains - half // 2 + m]

    sums = [s + outgoing[dom, pl.ds(q * fields, fields), :] for q, s in enumerate(sums)]
    stat = stat + outgoing[dom, pl.ds(body_rows, 1), :]
    pltpu.make_async_remote_copy(
        src_ref=stat_in,
        dst_ref=stat_in,
        send_sem=stat_send,
        recv_sem=stat_recv,
        device_id=(other, dom),
        device_id_type=MESH,
    ).wait_recv()
    stat = stat + jnp.sum(stat_in[...], axis=0)
    wait_all(1, half // 2)
    late, late_stat = gathered(range(half, half + half // 2))
    sums = [a + b for a, b in zip(sums, late)]
    stat = stat + late_stat
    for q in range(lane_tiles):
        cut = slice(q * 128, (q + 1) * 128)
        merged_ref[:, cut] = sums[q] * inverse[:, cut] + ocean_part[:, cut]

    mean = stat / pltpu.roll(stat, 64, 1)
    for c in range(groups + 1):
        moved = mean if c == 0 else pltpu.roll(mean, 128 - 16 * c, 1)
        means_ref[pl.ds(c, 1), :] = moved[:, :fields]

    pltpu.make_async_remote_copy(
        src_ref=rows_in.at[pl.ds(0, (domains - 1) * groups * lane_tiles)],
        dst_ref=rows_in.at[pl.ds(0, (domains - 1) * groups * lane_tiles)],
        send_sem=row_send,
        recv_sem=row_recv,
        device_id=(other, dom),
        device_id_type=MESH,
    ).wait_send()
    pltpu.make_async_remote_copy(
        src_ref=partner_in,
        dst_ref=partner_in,
        send_sem=pair_send,
        recv_sem=pair_recv.at[0],
        device_id=(other, dom),
        device_id_type=MESH,
    ).wait_send()
    pltpu.make_async_remote_copy(
        src_ref=stat_in,
        dst_ref=stat_in,
        send_sem=stat_send,
        recv_sem=stat_recv,
        device_id=(other, dom),
        device_id_type=MESH,
    ).wait_send()
    pltpu.make_async_remote_copy(
        src_ref=outgoing.at[pl.ds(0, domains - 1), pl.ds(0, body_rows + 1)],
        dst_ref=outgoing.at[pl.ds(0, domains - 1), pl.ds(0, body_rows + 1)],
        send_sem=main_send,
        recv_sem=main_recv.at[0],
        device_id=(other, dom),
        device_id_type=MESH,
    ).wait_send()


def finish(merged_in, means_in, merged_hbm, means_hbm, sem):
    copies = [
        pltpu.make_async_copy(merged_in, merged_hbm, sem.at[0]),
        pltpu.make_async_copy(means_in, means_hbm, sem.at[1]),
    ]
    for copy in copies:
        copy.start()
    for copy in copies:
        copy.wait()


def on_device(
    surface_flux,
    active_mask,
    source_area,
    tile_targets,
    remap_tiles,
    ocean_flux,
    air_fraction,
    air_area,
):
    groups = lax.axis_size("comp")
    domains = lax.axis_size("dom")
    owners = groups * domains
    fields = surface_flux.shape[1]
    cells = surface_flux.shape[2]
    blocks, slots, block_cells, air_cells = remap_tiles.shape
    lane_tiles = air_cells // 128
    message = -(-(lane_tiles * fields + 1) // 8) * 8
    vmem = pl.BlockSpec(memory_space=pltpu.VMEM)
    hbm = pl.BlockSpec(memory_space=pltpu.HBM)
    dma = pltpu.SemaphoreType.DMA
    parts = pl.pallas_call(
        functools.partial(kernel, groups, domains),
        out_shape=(
            pltpu.VMEM((fields, air_cells), F32),
            pltpu.VMEM((groups + 1, fields), F32),
        ),
        in_specs=[hbm] * 8,
        out_specs=(vmem, vmem),
        scratch_shapes=[
            pltpu.VMEM(surface_flux.shape, F32),
            pltpu.VMEM((1, cells), jnp.int32),
            pltpu.VMEM((1, cells), F32),
            pltpu.VMEM((slots, blocks), jnp.int32),
            pltpu.VMEM(remap_tiles.shape, F32),
            pltpu.VMEM(ocean_flux.shape, F32),
            pltpu.VMEM(air_fraction.shape, F32),
            pltpu.VMEM((air_cells,), F32),
            pltpu.VMEM((2 * fields, cells), F32),
            pltpu.VMEM((4 * fields, 2 * cells), BF16),
            pltpu.VMEM((lane_tiles, blocks * slots * fields, 128), F32),
            pltpu.VMEM((1, blocks * slots), jnp.int32),
            pltpu.VMEM((groups * lane_tiles, 128), F32),
            pltpu.VMEM((domains * 8, 128), F32),
            pltpu.VMEM((fields, owners, air_cells), F32),
            pltpu.VMEM((fields, 128), F32),
            pltpu.VMEM((fields, domains, air_cells), F32),
            pltpu.VMEM((1, 128), F32),
            pltpu.VMEM((domains, 1, 128), F32),
            pltpu.VMEM((domains, message, 128), F32),
            pltpu.VMEM((domains, message, 128), F32),
            pltpu.VMEM((domains // 4, message, 128), F32),
            dma((PARTS,)),
            dma((sum(len(c) for c in plan(blocks)[0]),)),
            dma((5,)),
            dma,
            dma,
            dma,
            dma((PAIR_CUTS,)),
            dma,
            dma,
            dma,
            dma((3 + domains // 4,)),
        ],
        compiler_params=pltpu.CompilerParams(
            collective_id=0, has_side_effects=True, vmem_limit_bytes=60 * 1024 * 1024
        ),
    )(
        surface_flux,
        active_mask.reshape(1, cells),
        source_area.reshape(1, cells),
        tile_targets.T,
        remap_tiles,
        ocean_flux,
        air_fraction,
        air_area,
    )
    return pl.pallas_call(
        finish,
        out_shape=(
            jax.ShapeDtypeStruct((fields, air_cells), F32),
            jax.ShapeDtypeStruct((groups + 1, fields), F32),
        ),
        in_specs=[vmem, vmem],
        out_specs=(hbm, hbm),
        scratch_shapes=[dma((2,))],
    )(*[pltpu.with_memory_space_constraint(p, pltpu.VMEM) for p in parts])


def solution(mesh):
    in_specs = (
        P(None, None, ("comp", "dom")),
        P(("comp", "dom")),
        P(("comp", "dom")),
        P(("comp", "dom"), None),
        P(("comp", "dom"), None, None, None),
        P(None, ("comp", "dom")),
        P(None, ("comp", "dom")),
        P(("comp", "dom")),
    )
    out_specs = (P(None, ("comp", "dom")), P())
    return jax.shard_map(
        on_device, mesh=mesh, in_specs=in_specs, out_specs=out_specs, check_vma=False
    )
```
